512 devices in a mesh: gx: 32 (over x, y_hi, core), gy: 16 (over z, y_lo).
Axes of the slice: x: 4, y: 8 (y_hi: 4, y_lo: 2; y = y_hi * 2 + y_lo), z: 8, core: 2. Of those that a mesh axis runs over, the one named last changes fastest.
Arguments:
- positions: float32 [3, 65536], P(None, ('gx', 'gy')), may hold values from 0 to 1
- species: int32 [65536], P(('gx', 'gy')), may hold values from 0 to 3
- neighbours: int32 [8, 65536], P(None, ('gx', 'gy')), may hold values from 0 to 639, as said below
- counts: int32 [65536], P(('gx', 'gy')), may hold values from 0 to 8, as said below
- live_atoms: int32 [512], P(('gx', 'gy')), may hold values from 64 to 128, as said below
- ghost_send: int32 [262144], P(('gx', 'gy')), may hold values from 0 to 127, as said below
- embed: float32 [128, 4], replicated, may hold values from -6 to 6
- site_energy: float32 [4], replicated, may hold values from -6 to 6
- radial_in: float32 [2, 64, 8], replicated, may hold values from -3 to 3
- radial_mid: float32 [2, 64, 64], replicated, may hold values from -1 to 1
- radial_out: float32 [2, 384, 64], replicated, may hold values from -1.5 to 1.5
- contract: float32 [2, 4, 6, 128], replicated, may hold values from -6 to 6
- mix: float32 [2, 128, 128], replicated, may hold values from -1 to 1
- skip: float32 [2, 128, 128], replicated, may hold values from -0.5 to 0.5
- read_one: float32 [128], replicated, may hold values from -1 to 1
- read_hidden: float32 [16, 128], replicated, may hold values from -1 to 1
- read_out: float32 [16], replicated, may hold values from -3 to 3
Outputs:
- energy: float32 [], replicated
- forces: float32 [3, 65536], P(None, ('gx', 'gy'))
- stress: float32 [3, 3], replicated
The draws below stay inside these ranges and needn't reach their ends.
Inputs may be any that keep to these rules, and one draw needn't show every extreme that they name: `live_atoms`: device 0 holds 128 real atoms. `counts`: zero for padding atoms; atom slot 0 of every device uses all 8 slots. `neighbours`: the used slots of an atom name a real atom of the same device (below its live count) or a ghost slot, numbered from 128 in the order of directions. `ghost_send`: each entry names a real atom of the sending device.
All inputs are finite; a program needn't handle non-finite values.
Results may differ from the reference program's by a relative error of at most 0.0003.
Values sent between devices are 32-bit elements; how exact they have to be, the bound alone decides.
A program may use at most 64 MiB of HBM per device.

```python
import jax
import jax.numpy as jnp
import numpy as np
from jax import lax

C = 128
H = 64
NB = 8
S = 4
RH = 16
K = 8
ATOM_DEV = 128
GHOST = 64
ATOMS = 65536
N_GX = 32
N_GY = 16


def live_table(key):
    device_total = ATOMS // ATOM_DEV
    table = jax.random.randint(jax.random.fold_in(key, 71), (device_total,), ATOM_DEV // 2, ATOM_DEV + 1)
    return table.at[0].set(ATOM_DEV)


def draw_live_atoms(key, part):
    return live_table(key)


def draw_counts(key, part):
    device_total = ATOMS // ATOM_DEV
    live = live_table(key)
    drawn = jax.random.randint(jax.random.fold_in(key, 72), (device_total, ATOM_DEV), K // 2, K + 1)
    drawn = jnp.where(jnp.arange(ATOM_DEV)[None, :] < live[:, None], drawn, 0)
    drawn = drawn.at[:, 0].set(K)
    return drawn.reshape(-1)


def draw_neighbours(key, part):
    device_total = ATOMS // ATOM_DEV
    live = live_table(key)
    limit = (live + 8 * GHOST)[None, :, None]
    drawn = jax.random.randint(jax.random.fold_in(key, 73), (K, device_total, ATOM_DEV), 0, limit)
    picked = jnp.where(drawn < live[None, :, None], drawn, drawn - live[None, :, None] + ATOM_DEV)
    return picked.reshape(K, -1)


def draw_ghost_send(key, part):
    device_total = ATOMS // ATOM_DEV
    live = live_table(key)
    drawn = jax.random.randint(jax.random.fold_in(key, 74), (device_total, 8 * GHOST), 0, live[:, None])
    return drawn.reshape(-1)


def set_ends(values, key, low, largest):
    longest = values.shape.index(max(values.shape))
    spots = []
    for shift in (0, 1):
        where = [jax.random.randint(jax.random.fold_in(key, axis), (), 0, length) for axis, length in enumerate(values.shape)]
        where[longest] = (where[longest] + shift) % values.shape[longest]
        spots.append(tuple(where))
    return values.at[spots[0]].set(low).at[spots[1]].set(largest)


def block_levels(stream_key, dims, pieces, smallest, high):
    def one(position, shards_of):
        steps = jax.random.uniform(jax.random.fold_in(jax.random.fold_in(stream_key, 6), position), (shards_of,), jnp.float32, smallest / len(pieces), high / len(pieces))
        return jnp.repeat(jnp.exp(steps), dims[position] // shards_of).reshape((-1,) + (1,) * (len(dims) - position - 1))

    loudness = one(*pieces[0])
    for cut in pieces[1:]:
        loudness = loudness * one(*cut)
    return loudness


def noise(key, extent, spread, most, held_as=jnp.bfloat16):
    values = jax.random.normal(key, extent, jnp.float32) * spread
    return jnp.minimum(jnp.maximum(values, -most), most).astype(held_as)


def setup_inputs(seed: int = 0) -> dict:
    splits = jax.random.split(jax.random.key(seed), 18)
    return {
        "positions": jnp.clip(1.0 * jax.random.uniform(splits[0], (3, ATOMS), jnp.float32) ** block_levels(splits[0], (3, ATOMS), ((1, 512),), -0.2, 0.2), 0.0, 1.0),
        "species": set_ends(jax.random.randint(splits[1], (ATOMS,), 0, S), jax.random.fold_in(splits[1], 1), 0, S - 1).astype(jnp.int32),
        "neighbours": draw_neighbours(jax.random.fold_in(splits[17], 71), 0),
        "counts": draw_counts(jax.random.fold_in(splits[17], 71), 0),
        "live_atoms": draw_live_atoms(jax.random.fold_in(splits[17], 71), 0),
        "ghost_send": draw_ghost_send(jax.random.fold_in(splits[17], 71), 0),
        "embed": noise(splits[6], (C, S), 1.0, 6.0, jnp.float32),
        "site_energy": noise(splits[7], (S,), 1.0, 6.0, jnp.float32),
        "radial_in": noise(splits[8], (2, H, NB), (NB // 2) ** -0.5, 3.0, jnp.float32),
        "radial_mid": noise(splits[9], (2, H, H), (H // 2) ** -0.5, 1.0, jnp.float32),
        "radial_out": noise(splits[10], (2, 3 * C, H), (H // 4) ** -0.5, 1.5, jnp.float32),
        "contract": noise(splits[11], (2, S, 6, C), 1.0, 6.0, jnp.float32),
        "mix": noise(splits[12], (2, C, C), (C // 4) ** -0.5, 1.0, jnp.float32),
        "skip": noise(splits[13], (2, C, C), C ** -0.5, 0.5, jnp.float32),
        "read_one": noise(splits[14], (C,), (C // 4) ** -0.5, 1.0, jnp.float32),
        "read_hidden": noise(splits[15], (RH, C), (C // 4) ** -0.5, 1.0, jnp.float32),
        "read_out": noise(splits[16], (RH,), (RH // 4) ** -0.5, 3.0, jnp.float32),
    }


highest = lax.Precision.HIGHEST
cut_sq = 4.0
span = 2.0
directions = ((-1, -1), (-1, 0), (-1, 1), (0, -1), (0, 1), (1, -1), (1, 0), (1, 1))

def edge_layer(edge_vec, valid, neigh_feat, self_feat, onehot, radial_in, radial_mid, radial_out, contract, mix, skip):
    slot_count, atom_count = valid.shape
    channels = mix.shape[0]
    basis_count = radial_in.shape[1]
    scaled = lax.optimization_barrier(jnp.sum(edge_vec * edge_vec, axis=0)) / cut_sq
    spacing = span / (basis_count - 1)
    centers = lax.iota(jnp.int32, basis_count).astype(jnp.float32) * spacing
    basis = jnp.exp(-0.5 * jnp.square((scaled[None] - centers[:, None, None]) / spacing))
    hidden = jax.nn.silu(jnp.dot(radial_in, basis.reshape(basis_count, slot_count * atom_count), precision=highest))
    hidden = jax.nn.silu(jnp.dot(radial_mid, hidden, precision=highest))
    radial = jnp.dot(radial_out, hidden, precision=highest).reshape(3, channels, slot_count, atom_count)
    radial = radial * (jnp.exp(-scaled) * valid)[None, None]
    weighted = radial * neigh_feat[None]
    comp_x, comp_y, comp_z = (edge_vec[0], edge_vec[1], edge_vec[2])
    harm_two = jnp.stack([comp_x * comp_y, comp_y * comp_z, comp_x * comp_z, 0.5 * (comp_x * comp_x - comp_y * comp_y), (2.0 * comp_z * comp_z - comp_x * comp_x - comp_y * comp_y) / 6.0])
    scalar_part = lax.optimization_barrier(jnp.sum(weighted[0], axis=1)) / slot_count
    vector_part = jnp.einsum('cka,mka->mca', weighted[1], edge_vec, precision=highest) / slot_count
    tensor_part = jnp.einsum('cka,mka->mca', weighted[2], harm_two, precision=highest) / slot_count
    square_one = lax.optimization_barrier(jnp.sum(vector_part * vector_part, axis=0))
    square_two = lax.optimization_barrier(jnp.sum(tensor_part * tensor_part, axis=0))
    tensor_xx = tensor_part[3] - tensor_part[4]
    tensor_yy = -tensor_part[3] - tensor_part[4]
    tensor_zz = 2.0 * tensor_part[4]
    triple = tensor_xx * vector_part[0] ** 2 + tensor_yy * vector_part[1] ** 2 + tensor_zz * vector_part[2] ** 2
    triple = triple + 2.0 * (tensor_part[0] * vector_part[0] * vector_part[1] + tensor_part[1] * vector_part[1] * vector_part[2] + tensor_part[2] * vector_part[0] * vector_part[2])
    paths = jnp.stack([scalar_part, scalar_part * scalar_part, square_one, square_two, scalar_part * square_one, triple])
    select = jnp.einsum('spc,sa->pca', contract, onehot, precision=highest)
    mixed = lax.optimization_barrier(jnp.sum(select * paths, axis=0))
    return jnp.dot(mix, mixed, precision=highest) + jnp.dot(skip, self_feat, precision=highest)

def local_setup(pos, kind, neigh, count, live, arrived, kinds):
    slot_count, atom_count = neigh.shape
    onehot_local = (kind[None, :] == lax.iota(jnp.int32, kinds)[:, None]).astype(jnp.float32)
    valid = (lax.iota(jnp.int32, slot_count)[:, None] < count[None, :]).astype(jnp.float32)
    live_mask = (lax.iota(jnp.int32, atom_count) < live).astype(jnp.float32)
    offsets = jnp.asarray(np.array([[heading[0] for heading in directions], [heading[1] for heading in directions], [0] * 8], np.float32))[:, :, None]
    ghost_pos = (arrived[0:3] + offsets).reshape(3, -1)
    ext_pos = jnp.concatenate([pos, ghost_pos], 1)
    edge_vec = ext_pos[:, neigh] - pos[:, None, :]
    ghost_kind = arrived[3].reshape(-1)
    onehot_ghost = (ghost_kind[None, :] == lax.iota(jnp.int32, kinds).astype(jnp.float32)[:, None]).astype(jnp.float32)
    onehot_ext = jnp.concatenate([onehot_local, onehot_ghost], 1)
    return (onehot_local, onehot_ext, valid, live_mask, edge_vec)

def layer_one(edge_vec, valid, onehot_local, onehot_ext, neigh, embed, weights):
    radial_in, radial_mid, radial_out, contract, mix, skip = weights
    start = jnp.dot(embed, onehot_ext, precision=highest)
    atom_count = valid.shape[1]
    return edge_layer(edge_vec, valid, start[:, neigh], start[:, :atom_count], onehot_local, radial_in[0], radial_mid[0], radial_out[0], contract[0], mix[0], skip[0])

def energy_two(edge_vec, neigh_feat, self_feat, valid, onehot_local, live_mask, weights, read_hidden, read_out):
    radial_in, radial_mid, radial_out, contract, mix, skip = weights
    second = edge_layer(edge_vec, valid, neigh_feat, self_feat, onehot_local, radial_in[1], radial_mid[1], radial_out[1], contract[1], mix[1], skip[1])
    site = jnp.dot(read_out, jax.nn.silu(jnp.dot(read_hidden, second, precision=highest)), precision=highest)
    return jnp.sum(site * live_mask)

def assemble(values, send):
    device_total, rows, atom_count = values.shape
    grid = values.reshape(N_GX, N_GY, rows, atom_count)
    send_grid = send.reshape(N_GX, N_GY, 8, GHOST)
    blocks = []
    for heading in range(8):
        shift_x, shift_y = directions[heading]
        source = jnp.roll(grid, (-shift_x, -shift_y), (0, 1))
        picks = jnp.roll(send_grid[:, :, heading], (-shift_x, -shift_y), (0, 1))
        blocks.append(jnp.take_along_axis(source, picks[:, :, None, :], axis=3))
    return jnp.stack(blocks, 3).reshape(device_total, rows, 8, GHOST)

def return_home(grads, send):
    device_total, rows = (grads.shape[0], grads.shape[1])
    grid = grads.reshape(N_GX, N_GY, rows, 8, GHOST)
    send_grid = send.reshape(N_GX, N_GY, 8, GHOST)
    total = jnp.zeros((device_total, rows, ATOM_DEV), jnp.float32)

    def place(block, picks):
        return jnp.zeros((rows, ATOM_DEV), jnp.float32).at[:, picks].add(block)
    for heading in range(8):
        shift_x, shift_y = directions[heading]
        moved = jnp.roll(grid[:, :, :, heading], (shift_x, shift_y), (0, 1)).reshape(device_total, rows, GHOST)
        picks = send_grid[:, :, heading].reshape(device_total, GHOST)
        total = total + jax.vmap(place)(moved, picks)
    return total

def reference(positions, species, neighbours, counts, live_atoms, ghost_send, embed, site_energy, radial_in, radial_mid, radial_out, contract, mix, skip, read_one, read_hidden, read_out):
    device_total = N_GX * N_GY
    weights = (radial_in, radial_mid, radial_out, contract, mix, skip)
    channels, kinds = embed.shape
    pos_dev = positions.reshape(3, device_total, ATOM_DEV).transpose(1, 0, 2)
    kind_dev = species.reshape(device_total, ATOM_DEV)
    neigh_dev = neighbours.reshape(K, device_total, ATOM_DEV).transpose(1, 0, 2)
    count_dev = counts.reshape(device_total, ATOM_DEV)
    send_dev = ghost_send.reshape(device_total, 8 * GHOST)
    packet_dev = jnp.concatenate([pos_dev, kind_dev[:, None, :].astype(jnp.float32)], 1)
    arrived_dev = assemble(packet_dev, send_dev)
    common = (pos_dev, kind_dev, neigh_dev, count_dev, live_atoms, arrived_dev)

    def first_pass(items):
        pos, kind, neigh, count, live, arrived = items
        onehot_local, onehot_ext, valid, live_mask, edge_vec = local_setup(pos, kind, neigh, count, live, arrived, kinds)
        return layer_one(edge_vec, valid, onehot_local, onehot_ext, neigh, embed, weights)
    first_dev = lax.map(first_pass, common)
    ghosts_dev = assemble(first_dev, send_dev)

    def second_pass(items):
        pos, kind, neigh, count, live, arrived, first, ghosts = items
        onehot_local, onehot_ext, valid, live_mask, edge_vec = local_setup(pos, kind, neigh, count, live, arrived, kinds)
        ext_first = jnp.concatenate([first, ghosts.reshape(channels, -1)], 1)

        def second(vec_in, neigh_in, self_in):
            return energy_two(vec_in, neigh_in, self_in, valid, onehot_local, live_mask, weights, read_hidden, read_out)
        energy_second, pullback = jax.vjp(second, edge_vec, ext_first[:, neigh], first)
        grad_vec, grad_neigh, grad_self = pullback(jnp.ones((), jnp.float32))
        ext_grad = jnp.zeros(ext_first.shape, jnp.float32).at[:, neigh].add(grad_neigh)
        atom_count = first.shape[1]
        own_grad = ext_grad[:, :atom_count] + grad_self + read_one[:, None] * live_mask[None, :]
        energy_first = jnp.sum(live_mask * (jnp.dot(read_one, first, precision=highest) + jnp.dot(site_energy, onehot_local, precision=highest)))
        return (energy_first + energy_second, grad_vec, own_grad, ext_grad[:, atom_count:].reshape(channels, 8, -1))
    energy_dev, grad_two_dev, own_dev, ghost_grad_dev = lax.map(second_pass, common + (first_dev, ghosts_dev))
    grad_first_dev = own_dev + return_home(ghost_grad_dev, send_dev)

    def third_pass(items):
        pos, kind, neigh, count, live, arrived, grad_first, grad_two = items
        onehot_local, onehot_ext, valid, live_mask, edge_vec = local_setup(pos, kind, neigh, count, live, arrived, kinds)

        def first_of(vec_in):
            return layer_one(vec_in, valid, onehot_local, onehot_ext, neigh, embed, weights)
        unused, pullback = jax.vjp(first_of, edge_vec)
        grad_vec = pullback(grad_first)[0] + grad_two
        atom_count = pos.shape[1]
        ext_pos_grad = jnp.zeros((3, onehot_ext.shape[1]), jnp.float32).at[:, neigh].add(grad_vec)
        own = ext_pos_grad[:, :atom_count] - lax.optimization_barrier(jnp.sum(grad_vec, axis=1))
        virial = jnp.einsum('ika,jka->ij', edge_vec, grad_vec, precision=highest)
        return (own, ext_pos_grad[:, atom_count:].reshape(3, 8, -1), virial)
    own_pos, ghost_pos_grad, virial_dev = lax.map(third_pass, common + (grad_first_dev, grad_two_dev))
    pos_grad = own_pos + return_home(ghost_pos_grad, send_dev)
    forces = -pos_grad.transpose(1, 0, 2).reshape(3, -1)
    live_total = jnp.sum(live_atoms).astype(jnp.float32)
    energy = jnp.sum(energy_dev) / live_total
    stress = lax.optimization_barrier(jnp.sum(virial_dev, axis=0)) / live_total
    return (energy, forces, stress)
```

```python
import functools

import jax
import jax.numpy as jnp
from jax import lax
from jax.experimental import pallas as pl
from jax.experimental.pallas import tpu as pltpu
from jax.sharding import PartitionSpec as P

F32 = jnp.float32
BF = jnp.bfloat16
C = 128
H = 64
K = 8
A = 128
E = K * A
G = 512
DIRS = ((-1, -1), (-1, 0), (-1, 1), (0, -1), (0, 1), (1, -1), (1, 0), (1, 1))
NX, NYH, NCORE = 4, 4, 2
NZ, NYL = 8, 2
SPACING = 2.0 / 7.0


def dot(a, b):
    return lax.dot_general(a, b, (((1,), (0,)), ((), ())), preferred_element_type=F32)


def dot_nt(a, b):
    return lax.dot_general(a, b, (((1,), (1,)), ((), ())), preferred_element_type=F32)


def dot_tn(a, b):
    return lax.dot_general(a, b, (((0,), (0,)), ((), ())), preferred_element_type=F32)


def split2(x):
    hi = x.astype(BF)
    return hi, (x - hi.astype(F32)).astype(BF)


def split3(x):
    hi = x.astype(BF).astype(F32)
    rest = x - hi
    mid = rest.astype(BF).astype(F32)
    return hi, mid, rest - mid


def dot3(a, b):
    ah, al = split2(a)
    bh, bl = split2(b)
    return dot(ah, bh) + (dot(ah, bl) + dot(al, bh))


def stack3(x):
    hi, lo = split2(x)
    return jnp.concatenate([hi, lo, hi], 0)


def iota(shape, axis):
    return lax.broadcasted_iota(jnp.int32, shape, axis)


def eye(n, dtype=BF):
    return (iota((n, n), 0) == iota((n, n), 1)).astype(F32).astype(dtype)


def spread3(w):
    n = w.shape[1]
    hi, lo = split2(w)
    row, col = iota((n, 3 * n), 0), iota((n, 3 * n), 1)
    first = ((col == row) | (col == row + n)).astype(F32).astype(BF)
    last = (col == row + 2 * n).astype(F32).astype(BF)
    return (dot(hi, first) + dot(lo, last)).astype(BF)


def transpose2(w):
    hi, lo = split2(w)
    unit = eye(w.shape[1])
    return dot_nt(unit, hi).astype(BF), dot_nt(unit, lo).astype(BF)


def rows3(x):
    hi, mid, lo = split3(x)
    return jnp.concatenate([hi, mid, lo, jnp.zeros_like(hi)], 0).astype(BF)


def fold3(y):
    return y[0:8] + (y[8:16] + y[16:24])


def fold2(y):
    n = y.shape[0] // 2
    return y[:n] + y[n:]


def tile_lanes(x, count):
    return jnp.concatenate([x] * count, 1)


def twice(x):
    return jnp.concatenate([x, x], 0)


def kernel(
    live_ref, pos_ref, kind_ref, neigh_ref, count_ref, send_ref, embed_ref, site_ref, win_ref,
    wmid_ref, wout_ref, contract_ref, mix_ref, skip_ref, rone_ref, rhid_ref, rout_ref,
    energy_ref, forces_ref, stress_ref,
    s_ref, st_ref, oh_ref, oht_ref,
    snd1, rcv1, snd2, rcv2, snd3, rcv3, snd4, rcv4, ar1s, ar1r, ar2s, ar2r, ar3s, ar3r,
    rad_ref, feat_ref, hb_ref, a_ref, sel_ref, da_ref, dr_ref, gn_ref, d1_ref, d2_ref, hid_ref,
    bas_ref, wic_ref, wmc_ref, woc_ref, wot_ref, wmt_ref, wit_ref, mixc_ref, mixt_ref, mixed_ref,
    edge_ref, dh_ref,
    ss1, rs1, ss2, rs2, ss3, rs3, ss4, rs4, sa1, ra1, sa2, ra2, sa3, ra3,
):
    p = lax.axis_index("gx")
    q = lax.axis_index("gy")
    n_gx = NX * NYH * NCORE
    n_gy = NZ * NYL

    def near(ox, oy):
        return (lax.rem(p + (ox + n_gx), n_gx), lax.rem(q + (oy + n_gy), n_gy))

    core = lax.rem(p, NCORE)
    y_hi = lax.rem(lax.div(p, NCORE), NYH)
    x = lax.div(p, NCORE * NYH)
    y_lo = lax.rem(q, NYL)
    z = lax.div(q, NYL)
    y = y_hi * NYL + y_lo

    def peer_a(i):
        dx, dc = i // NCORE, i % NCORE
        return ((lax.rem(x + dx, NX) * NYH + y_hi) * NCORE + lax.rem(core + dc, NCORE), q)

    def peer_b(i):
        yy = lax.rem(y + i, NYH * NYL)
        return ((x * NYH + lax.div(yy, NYL)) * NCORE + core, z * NYL + lax.rem(yy, NYL))

    def peer_c(i):
        return (p, lax.rem(z + i, NZ) * NYL + y_lo)

    peers_a = [peer_a(i) for i in range(1, NX * NCORE)]
    peers_b = [peer_b(i) for i in range(1, NYH * NYL)]
    peers_c = [peer_c(i) for i in range(1, NZ)]
    ahead = [near(ox, oy) for ox, oy in DIRS]
    back = [near(-ox, -oy) for ox, oy in DIRS]

    barrier = pltpu.get_barrier_semaphore()
    everyone = ahead + peers_a + peers_b + peers_c
    for who in everyone:
        pl.semaphore_signal(barrier, inc=1, device_id=who, device_id_type=pl.DeviceIdType.MESH)

    def remote(src, dst, ssem, rsem, who):
        return pltpu.make_async_remote_copy(
            src_ref=src, dst_ref=dst, send_sem=ssem, recv_sem=rsem, device_id=who,
            device_id_type=pl.DeviceIdType.MESH,
        )

    half = iota((8, 128), 1) < 64

    for b in range(4):
        row = send_ref[0:1, b * 128 : (b + 1) * 128]
        s_ref[:, b * 128 : (b + 1) * 128] = (iota((A, 128), 0) == row).astype(F32).astype(BF)
    kind = kind_ref[0:1, :]
    own8 = jnp.concatenate([pos_ref[...], kind.astype(F32), jnp.zeros((4, A), F32)], 0)
    own32 = rows3(own8)
    packet = fold3(dot(own32, s_ref[...]))
    for b in range(4):
        snd1[b] = packet[:, b * 128 : (b + 1) * 128]

    pl.semaphore_wait(barrier, len(everyone))
    copies1 = [remote(snd1.at[o // 2], rcv1.at[o], ss1.at[o], rs1.at[o], back[o]) for o in range(8)]
    for copy in copies1:
        copy.start()

    for k in range(K):
        row = neigh_ref[k : k + 1, :]
        oh_ref[:, k * A : (k + 1) * A] = (iota((A + G, A), 0) == row).astype(F32).astype(BF)
    unit = eye(128)
    for k in range(K):
        for b in range(5):
            block = oh_ref[b * 128 : (b + 1) * 128, k * A : (k + 1) * A]
            oht_ref[k * A : (k + 1) * A, b * 128 : (b + 1) * 128] = dot_tn(block, unit).astype(BF)
    for b in range(4):
        st_ref[b * 128 : (b + 1) * 128, :] = dot_tn(s_ref[:, b * 128 : (b + 1) * 128], unit).astype(BF)

    kinds4 = iota((16, A), 0)
    onehot16 = ((lax.rem(kinds4, 4) == kind) & (kinds4 < 12)).astype(F32).astype(BF)
    for l in range(2):
        in_h = win_ref[l].astype(BF).astype(F32)
        in_rows = jnp.concatenate([in_h, in_h, win_ref[l] - in_h, jnp.zeros_like(in_h)], 0)
        wic_ref[l] = dot_tn(in_rows.astype(BF), eye(32)).astype(BF)
        wmc_ref[l] = spread3(wmid_ref[l])
        oh_t, ol_t = split2(wout_ref[l])
        wot_ref[l] = jnp.concatenate([oh_t, ol_t], 0)
        woc_ref[l] = dot_tn(jnp.concatenate([oh_t, oh_t, ol_t], 0), eye(3 * H)).astype(BF)
        mh_t, ml_t = transpose2(wmid_ref[l])
        wmt_ref[l] = spread3(mh_t.astype(F32) + ml_t.astype(F32))
        wit_ref[l] = spread3(win_ref[l])
        parts = []
        for path in range(6):
            hi, mid, lo = split3(contract_ref[l, path])
            parts.append(jnp.concatenate([hi, mid, lo, jnp.zeros_like(hi)], 0).astype(BF))
        sel_ref[l] = dot_tn(jnp.concatenate(parts, 1), onehot16)
    mixh, mixl = split2(mix_ref[0])
    mixc_ref[...] = jnp.concatenate([mixh, mixh, mixl], 1)
    mth, mtl = transpose2(mix_ref[0])
    mixt_ref[...] = jnp.concatenate([mth, mth, mtl], 1)
    eh, em, el = split3(embed_ref[...])
    embed_rows = jnp.concatenate([eh, em, el, jnp.zeros_like(eh)], 0).astype(BF)
    embed16 = dot_tn(embed_rows, eye(16)).astype(BF)
    start_own = dot(embed16, onehot16)
    skip_start = dot3(skip_ref[0], start_own)
    read_mix = dot3(rhid_ref[...], mix_ref[1])
    read_skip = dot3(rhid_ref[...], skip_ref[1])
    rm_h, rm_l = split2(read_mix)
    rmc = jnp.concatenate([rm_h, rm_h, rm_l], 1)
    live_row = (iota((1, A), 1) < live_ref[...]).astype(F32)
    site_row = jnp.zeros((1, A), F32)
    for s in range(4):
        site_row = jnp.where(kind == s, site_ref[0:1, s : s + 1], site_row)

    gathered = fold3(dot(own32, oh_ref[0:A, :]))
    for copy in copies1:
        copy.wait()
    blocks = []
    rows8 = iota((8, 128), 0)
    for b in range(4):
        (ax, ay), (bx, by) = DIRS[2 * b], DIRS[2 * b + 1]
        shift_x = jnp.where(half, float(ax), float(bx))
        shift_y = jnp.where(half, float(ay), float(by))
        shift = jnp.where(rows8 == 0, shift_x, jnp.where(rows8 == 1, shift_y, 0.0))
        blocks.append(jnp.where(half, rcv1[2 * b], rcv1[2 * b + 1]) + shift)
    ghosts8 = jnp.concatenate(blocks, 1)
    gathered = gathered + fold3(dot(rows3(ghosts8), oh_ref[A:, :]))
    own_base = jnp.where(rows8 < 3, own8, 0.0)
    edge = gathered - tile_lanes(own_base, K)
    edge_ref[...] = edge
    ex, ey, ez = edge[0:1], edge[1:2], edge[2:3]
    spec_row = edge[3:4]
    scaled = (ex * ex + ey * ey + ez * ez) * 0.25
    valid = jnp.concatenate([(k < count_ref[0:1, :]).astype(F32) for k in range(K)], 1)
    cut = jnp.exp(-scaled) * valid * 0.125
    offset = (scaled - iota((8, E), 0).astype(F32) * SPACING) / SPACING
    basis = jnp.exp(-0.5 * (offset * offset))
    slope = basis * (offset * (-1.0 / SPACING))
    bh = basis.astype(BF).astype(F32)
    bas_ref[...] = jnp.concatenate([bh, basis - bh, bh, jnp.zeros_like(bh)], 0).astype(BF)

    def radial(l):
        pre = dot(wic_ref[l], bas_ref[...])
        sig = jax.nn.sigmoid(pre)
        act = pre * sig
        d1_ref[l] = sig + act * (1.0 - sig)
        pre = dot(wmc_ref[l], stack3(act))
        sig = jax.nn.sigmoid(pre)
        act = pre * sig
        d2_ref[l] = sig + act * (1.0 - sig)
        hid_ref[l] = act
        rad_ref[l] = dot(woc_ref[l], stack3(act * cut))

    radial(0)
    kinds_e = iota((16, E), 0)
    onehot_e = ((lax.rem(kinds_e, 4).astype(F32) == spec_row) & (kinds_e < 12)).astype(F32).astype(BF)
    feat_ref[0] = dot(embed16, onehot_e)
    harmonics = [
        ex, ey, ez, ex * ey, ey * ez, ex * ez, 0.5 * (ex * ex - ey * ey),
        (2.0 * ez * ez - ex * ex - ey * ey) / 6.0,
    ]
    for m in range(8):
        hb_ref[m * 8 : (m + 1) * 8, :] = jnp.broadcast_to(harmonics[m], (8, E))

    def harm(m, at):
        return twice(hb_ref[m * 8 : (m + 1) * 8, at])

    def moments(l):
        def body(block, carry):
            c0 = pl.multiple_of(block * 16, 16)
            total = None
            for k in range(K):
                at = slice(k * A, (k + 1) * A)
                h = feat_ref[l, pl.ds(c0, 16), at]
                w0 = rad_ref[l, pl.ds(c0, 16), at] * h
                w1 = rad_ref[l, pl.ds(C + c0, 16), at] * h
                w2 = rad_ref[l, pl.ds(2 * C + c0, 16), at] * h
                terms = [w0]
                terms += [w1 * harm(m, at) for m in range(3)]
                terms += [w2 * harm(m, at) for m in range(3, 8)]
                total = terms if total is None else [t + u for t, u in zip(total, terms)]
            for m in range(9):
                a_ref[l, pl.ds(m * C + c0, 16), :] = total[m]
            a0, x1, y1, z1, xy, yz, xz, u, w = total
            q1 = x1 * x1 + y1 * y1 + z1 * z1
            q2 = xy * xy + yz * yz + xz * xz + u * u + w * w
            triple = (u - w) * (x1 * x1) - (u + w) * (y1 * y1) + 2.0 * w * (z1 * z1)
            triple = triple + 2.0 * (xy * (x1 * y1) + yz * (y1 * z1) + xz * (x1 * z1))
            s = [sel_ref[l, pl.ds(path * C + c0, 16), :] for path in range(6)]
            mixed = s[0] * a0 + s[1] * (a0 * a0) + s[2] * q1 + s[3] * q2 + s[4] * (a0 * q1) + s[5] * triple
            hi, lo = split2(mixed)
            mixed_ref[pl.ds(c0, 16), :] = hi
            mixed_ref[pl.ds(C + c0, 16), :] = lo
            mixed_ref[pl.ds(2 * C + c0, 16), :] = hi
            return carry

        lax.fori_loop(0, C // 16, body, 0)

    def moment_grads(l, block, dm):
        c0 = pl.multiple_of(block * 16, 16)
        a0, x1, y1, z1, xy, yz, xz, u, w = [a_ref[l, pl.ds(m * C + c0, 16), :] for m in range(9)]
        g = [dm * sel_ref[l, pl.ds(path * C + c0, 16), :] for path in range(6)]
        q1 = x1 * x1 + y1 * y1 + z1 * z1
        g5 = 2.0 * g[5]
        dq = 2.0 * (g[2] + a0 * g[4])
        g3 = 2.0 * g[3]
        return [
            g[0] + 2.0 * (a0 * g[1]) + q1 * g[4],
            x1 * dq + g5 * ((u - w) * x1 + xy * y1 + xz * z1),
            y1 * dq + g5 * (xy * x1 - (u + w) * y1 + yz * z1),
            z1 * dq + g5 * (xz * x1 + yz * y1 + 2.0 * (w * z1)),
            xy * g3 + g5 * (x1 * y1),
            yz * g3 + g5 * (y1 * z1),
            xz * g3 + g5 * (x1 * z1),
            u * g3 + g[5] * (x1 * x1 - y1 * y1),
            w * g3 + g[5] * (2.0 * (z1 * z1) - x1 * x1 - y1 * y1),
        ]

    def weight_grads(d, at):
        w1 = d[1] * harm(0, at) + d[2] * harm(1, at) + d[3] * harm(2, at)
        w2 = d[4] * harm(3, at) + d[5] * harm(4, at) + d[6] * harm(5, at)
        return d[0], w1, w2 + (d[7] * harm(6, at) + d[8] * harm(7, at))

    def radial_grads(l):
        def body(k, carry):
            at = pl.ds(pl.multiple_of(k * A, A), A)
            hs = [harm(m, at) for m in range(8)]
            acc = [jnp.zeros((16, A), F32)] * 8
            for block in range(C // 16):
                c0 = block * 16
                d = [da_ref[m * C + c0 : m * C + c0 + 16, :] for m in range(9)]
                h = feat_ref[l, c0 : c0 + 16, at]
                w1 = rad_ref[l, C + c0 : C + c0 + 16, at] * h
                w2 = rad_ref[l, 2 * C + c0 : 2 * C + c0 + 16, at] * h
                e1 = d[1] * hs[0] + d[2] * hs[1] + d[3] * hs[2]
                e2 = d[4] * hs[3] + d[5] * hs[4] + d[6] * hs[5] + (d[7] * hs[6] + d[8] * hs[7])
                for n, value in enumerate((d[0], e1, e2)):
                    hi, lo = split2(value * h)
                    dr_ref[n * C + c0 : n * C + c0 + 16, at] = hi
                    dr_ref[3 * C + n * C + c0 : 3 * C + n * C + c0 + 16, at] = lo
                acc = [acc[m] + (w1 if m < 3 else w2) * d[m + 1] for m in range(8)]
            for m in range(8):
                dh_ref[m : m + 1, at] = jnp.sum(acc[m], axis=0, keepdims=True)
            return carry

        lax.fori_loop(0, K, body, 0)
        hi_part = dot(wot_ref[l], dr_ref[0 : 3 * C, :])
        dhc = fold2(hi_part) + dot(wot_ref[l, 0:H, :], dr_ref[3 * C :, :])
        dcut = jnp.sum(dhc * hid_ref[l], axis=0, keepdims=True)
        dpre = dhc * cut * d2_ref[l]
        dpre = dot(wmt_ref[l], stack3(dpre)) * d1_ref[l]
        dbasis = dot(wit_ref[l], stack3(dpre))
        ds = jnp.sum(dbasis * slope, axis=0, keepdims=True) - cut * dcut
        ds = ds * 0.5
        g0, g1, g2, g3, g4, g5, g6, g7 = [dh_ref[m : m + 1, :] for m in range(8)]
        third = g7 * (1.0 / 3.0)
        gx = g0 + ey * g3 + ez * g5 + ex * (g6 - third + ds)
        gy = g1 + ex * g3 + ez * g4 + ey * (ds - g6 - third)
        gz = g2 + ey * g4 + ex * g5 + ez * (2.0 * third + ds)
        return jnp.concatenate([gx, gy, gz, jnp.zeros((5, E), F32)], 0)

    moments(0)
    first = dot(mixc_ref[...], mixed_ref[...]) + skip_start

    first_h, first_l = split2(first)
    first2 = jnp.concatenate([first_h, first_l], 0)
    lane64 = iota((64, 128), 1) < 64

    def pack(value, buf):
        for b in range(4):
            top = value[0:64, b * 128 : (b + 1) * 128]
            low = value[64:128, b * 128 : (b + 1) * 128]
            buf[2 * b] = jnp.where(lane64, top, pltpu.roll(low, 64, 1))
            buf[2 * b + 1] = jnp.where(lane64, pltpu.roll(top, 64, 1), low)

    def unpack(buf, b):
        one, two = buf[2 * b], buf[2 * b + 1]
        top = jnp.where(lane64, one, pltpu.roll(two, 64, 1))
        low = jnp.where(lane64, pltpu.roll(one, 64, 1), two)
        return jnp.concatenate([top, low], 0)

    def unpack_all(buf):
        return jnp.concatenate([unpack(buf, b) for b in range(4)], 1)

    pack(fold2(dot(first2, s_ref[...])), snd2)
    copies2 = [remote(snd2.at[o], rcv2.at[o], ss2.at[o], rs2.at[o], back[o]) for o in range(8)]
    for copy in copies2:
        copy.start()

    radial(1)
    feat_ref[1] = fold2(dot(first2, oh_ref[0:A, :]))
    read_base = dot3(read_skip, first)
    energy_row = live_row * (dot3(rone_ref[...], first) + site_row)

    for copy in copies2:
        copy.wait()
    gh, gl = split2(unpack_all(rcv2))
    feat_ref[1] += fold2(dot(jnp.concatenate([gh, gl], 0), oh_ref[A:, :]))

    moments(1)
    pre = dot(rmc, mixed_ref[...]) + read_base
    sig = jax.nn.sigmoid(pre)
    act = pre * sig
    rout = jnp.sum(jnp.where(iota((16, 16), 0) == iota((16, 16), 1), rout_ref[...], 0.0), axis=1, keepdims=True)
    energy_row = energy_row + live_row * jnp.sum(rout * act, axis=0, keepdims=True)
    dpre = rout * live_row * (sig + act * (1.0 - sig))
    dph, dpl = split2(dpre)
    dmixed = dot_tn(rm_h, dph) + (dot_tn(rm_h, dpl) + dot_tn(rm_l, dph))

    def neigh_body(block, carry):
        c0 = pl.multiple_of(block * 16, 16)
        d = moment_grads(1, block, da_ref[pl.ds(9 * C + c0, 16), :])
        for m in range(9):
            da_ref[pl.ds(m * C + c0, 16), :] = d[m]
        for k in range(K):
            at = slice(k * A, (k + 1) * A)
            w0, w1, w2 = weight_grads(d, at)
            g = w0 * rad_ref[1, pl.ds(c0, 16), at]
            g = g + w1 * rad_ref[1, pl.ds(C + c0, 16), at]
            g = g + w2 * rad_ref[1, pl.ds(2 * C + c0, 16), at]
            hi, lo = split2(g)
            gn_ref[pl.ds(c0, 16), at] = hi
            gn_ref[pl.ds(C + c0, 16), at] = lo
        return carry

    da_ref[9 * C :, :] = dmixed
    lax.fori_loop(0, C // 16, neigh_body, 0)
    pack(fold2(dot(gn_ref[...], oht_ref[:, A:])), snd3)
    copies3 = [remote(snd3.at[o], rcv3.at[o], ss3.at[o], rs3.at[o], ahead[o]) for o in range(8)]
    for copy in copies3:
        copy.start()

    own_grad = fold2(dot(gn_ref[...], oht_ref[:, 0:A]))
    rs_h, rs_l = split2(read_skip)
    own_grad = own_grad + dot_tn(rs_h, dph) + (dot_tn(rs_h, dpl) + dot_tn(rs_l, dph))
    o_h, o_m, o_l = split3(jnp.concatenate([rone_ref[...], jnp.zeros((7, C), F32)], 0))
    live8 = jnp.where(rows8 == 0, live_row, 0.0).astype(BF)
    own_grad = own_grad + dot_tn(o_h.astype(BF), live8)
    own_grad = own_grad + (dot_tn(o_m.astype(BF), live8) + dot_tn(o_l.astype(BF), live8))
    grad_two = radial_grads(1)

    for copy in copies3:
        copy.wait()
    rh, rl = split2(unpack_all(rcv3))
    grad_first = own_grad + fold2(dot(jnp.concatenate([rh, rl], 0), st_ref[...]))
    da_ref[9 * C :, :] = dot(mixt_ref[...], stack3(grad_first))

    def first_body(block, carry):
        c0 = pl.multiple_of(block * 16, 16)
        d = moment_grads(0, block, da_ref[pl.ds(9 * C + c0, 16), :])
        for m in range(9):
            da_ref[pl.ds(m * C + c0, 16), :] = d[m]
        return carry

    lax.fori_loop(0, C // 16, first_body, 0)
    grad = radial_grads(0) + grad_two

    sums = []
    for b in range(3):
        prod = edge * grad[b : b + 1]
        part = prod[:, 0:A]
        for k in range(1, K):
            part = part + prod[:, k * A : (k + 1) * A]
        if b == 0:
            part = jnp.where(rows8 == 3, energy_row, jnp.where(rows8 == 4, live_row, part))
        sums.append(jnp.sum(part, axis=1, keepdims=True))
    lanes8 = iota((8, 128), 1)
    total = jnp.where(lanes8 == 0, sums[0], jnp.where(lanes8 == 1, sums[1], sums[2]))
    ar1s[...] = total

    def spread(src, dst, ssem, rsem, peers):
        copies = [remote(src, dst.at[i], ssem.at[i], rsem.at[i], who) for i, who in enumerate(peers)]
        for copy in copies:
            copy.start()
        return copies

    def gather_sum(base, buf, copies):
        for i, copy in enumerate(copies):
            copy.wait()
        for i in range(len(copies)):
            base = base + buf[i]
        return base

    reduce1 = spread(ar1s, ar1r, sa1, ra1, peers_a)

    g32 = rows3(grad)
    ghost_pos = fold3(dot(g32, oht_ref[:, A:]))
    for b in range(4):
        snd4[b] = ghost_pos[:, b * 128 : (b + 1) * 128]
    copies4 = [remote(snd4.at[o // 2], rcv4.at[o], ss4.at[o], rs4.at[o], ahead[o]) for o in range(8)]
    for copy in copies4:
        copy.start()
    own_pos = fold3(dot(g32, oht_ref[:, 0:A]))
    for k in range(K):
        own_pos = own_pos - grad[:, k * A : (k + 1) * A]

    total = gather_sum(total, ar1r, reduce1)
    ar2s[...] = total
    reduce2 = spread(ar2s, ar2r, sa2, ra2, peers_b)

    for copy in copies4:
        copy.wait()
    home = jnp.concatenate([jnp.where(half, rcv4[2 * b], rcv4[2 * b + 1]) for b in range(4)], 1)
    own_pos = own_pos + fold3(dot(rows3(home), st_ref[...]))
    forces_ref[...] = -own_pos[0:3]

    total = gather_sum(total, ar2r, reduce2)
    ar3s[...] = total
    reduce3 = spread(ar3s, ar3r, sa3, ra3, peers_c)
    total = gather_sum(total, ar3r, reduce3)
    count = total[4:5, 0:1]
    energy_ref[...] = total[3:4, 0:1] / count
    stress_ref[...] = total[0:3, 0:3] / count


def per_device(
    positions, species, neighbours, counts, live_atoms, ghost_send, embed, site_energy, radial_in,
    radial_mid, radial_out, contract, mix, skip, read_one, read_hidden, read_out,
):
    vmem = pl.BlockSpec(memory_space=pltpu.VMEM)
    dma = pltpu.SemaphoreType.DMA
    energy, forces, stress = pl.pallas_call(
        kernel,
        out_shape=(
            jax.ShapeDtypeStruct((1, 1), F32),
            jax.ShapeDtypeStruct((3, A), F32),
            jax.ShapeDtypeStruct((3, 3), F32),
        ),
        in_specs=[vmem] * 17,
        out_specs=(vmem, vmem, vmem),
        scratch_shapes=[
            pltpu.VMEM((A, G), BF),
            pltpu.VMEM((G, A), BF),
            pltpu.VMEM((A + G, E), BF),
            pltpu.VMEM((E, A + G), BF),
            pltpu.VMEM((4, 8, 128), F32),
            pltpu.VMEM((8, 8, 128), F32),
            pltpu.VMEM((8, 64, 128), F32),
            pltpu.VMEM((8, 64, 128), F32),
            pltpu.VMEM((8, 64, 128), F32),
            pltpu.VMEM((8, 64, 128), F32),
            pltpu.VMEM((4, 8, 128), F32),
            pltpu.VMEM((8, 8, 128), F32),
            pltpu.VMEM((8, 128), F32),
            pltpu.VMEM((7, 8, 128), F32),
            pltpu.VMEM((8, 128), F32),
            pltpu.VMEM((7, 8, 128), F32),
            pltpu.VMEM((8, 128), F32),
            pltpu.VMEM((7, 8, 128), F32),
            pltpu.VMEM((2, 3 * C, E), F32),
            pltpu.VMEM((2, C, E), F32),
            pltpu.VMEM((64, E), F32),
            pltpu.VMEM((2, 9 * C, A), F32),
            pltpu.VMEM((2, 6 * C, A), F32),
            pltpu.VMEM((10 * C, A), F32),
            pltpu.VMEM((6 * C, E), BF),
            pltpu.VMEM((2 * C, E), BF),
            pltpu.VMEM((2, H, E), F32),
            pltpu.VMEM((2, H, E), F32),
            pltpu.VMEM((2, H, E), F32),
            pltpu.VMEM((32, E), BF),
            pltpu.VMEM((2, H, 32), BF),
            pltpu.VMEM((2, H, 3 * H), BF),
            pltpu.VMEM((2, 3 * C, 3 * H), BF),
            pltpu.VMEM((2, 2 * H, 3 * C), BF),
            pltpu.VMEM((2, H, 3 * H), BF),
            pltpu.VMEM((2, 8, 3 * H), BF),
            pltpu.VMEM((C, 3 * C), BF),
            pltpu.VMEM((C, 3 * C), BF),
            pltpu.VMEM((3 * C, A), BF),
            pltpu.VMEM((8, E), F32),
            pltpu.VMEM((8, E), F32),
            dma((8,)), dma((8,)), dma((8,)), dma((8,)), dma((8,)), dma((8,)), dma((8,)), dma((8,)),
            dma((7,)), dma((7,)), dma((7,)), dma((7,)), dma((7,)), dma((7,)),
        ],
        compiler_params=pltpu.CompilerParams(
            collective_id=0, has_side_effects=True, vmem_limit_bytes=56 * 1024 * 1024
        ),
    )(
        live_atoms.reshape(1, 1), positions, species.reshape(1, A), neighbours, counts.reshape(1, A),
        ghost_send.reshape(1, G), embed.T, site_energy.reshape(1, 4), radial_in.transpose(0, 2, 1),
        radial_mid, radial_out.transpose(0, 2, 1), contract.transpose(0, 2, 1, 3), mix, skip,
        read_one.reshape(1, C), read_hidden, read_out.reshape(1, 16),
    )
    return energy.reshape(()), forces, stress


def solution(mesh):
    both = ("gx", "gy")
    placed = (P(None, both), P(both), P(None, both), P(both), P(both), P(both)) + (P(),) * 11
    return jax.shard_map(
        per_device, mesh=mesh, in_specs=placed, out_specs=(P(), P(None, both), P()), check_vma=False
    )
```

```python
import functools

import jax
import jax.numpy as jnp
from jax import lax
from jax.experimental import pallas as pl
from jax.experimental.pallas import tpu as pltpu
from jax.sharding import PartitionSpec as P

F32 = jnp.float32
BF = jnp.bfloat16
C = 128
H = 64
K = 8
A = 128
E = K * A
G = 512
DIRS = ((-1, -1), (-1, 0), (-1, 1), (0, -1), (0, 1), (1, -1), (1, 0), (1, 1))
NX, NYH, NCORE = 4, 4, 2
NZ, NYL = 8, 2
SPACING = 2.0 / 7.0


def dot(a, b):
    return lax.dot_general(a, b, (((1,), (0,)), ((), ())), preferred_element_type=F32)


def dot_nt(a, b):
    return lax.dot_general(a, b, (((1,), (1,)), ((), ())), preferred_element_type=F32)


def dot_tn(a, b):
    return lax.dot_general(a, b, (((0,), (0,)), ((), ())), preferred_element_type=F32)


def split2(x):
    hi = x.astype(BF)
    return hi, (x - hi.astype(F32)).astype(BF)


def split3(x):
    hi = x.astype(BF).astype(F32)
    rest = x - hi
    mid = rest.astype(BF).astype(F32)
    return hi, mid, rest - mid


def dot3(a, b):
    ah, al = split2(a)
    bh, bl = split2(b)
    return dot(ah, bh) + (dot(ah, bl) + dot(al, bh))


def stack3(x):
    hi, lo = split2(x)
    return jnp.concatenate([hi, lo, hi], 0)


def iota(shape, axis):
    return lax.broadcasted_iota(jnp.int32, shape, axis)


def eye(n, dtype=BF):
    return (iota((n, n), 0) == iota((n, n), 1)).astype(F32).astype(dtype)


def spread3(w):
    n = w.shape[1]
    hi, lo = split2(w)
    row, col = iota((n, 3 * n), 0), iota((n, 3 * n), 1)
    first = ((col == row) | (col == row + n)).astype(F32).astype(BF)
    last = (col == row + 2 * n).astype(F32).astype(BF)
    return (dot(hi, first) + dot(lo, last)).astype(BF)


def transpose2(w):
    hi, lo = split2(w)
    unit = eye(w.shape[1])
    return dot_nt(unit, hi).astype(BF), dot_nt(unit, lo).astype(BF)


def rows3(x):
    hi, mid, lo = split3(x)
    return jnp.concatenate([hi, mid, lo, jnp.zeros_like(hi)], 0).astype(BF)


def fold3(y):
    return y[0:8] + (y[8:16] + y[16:24])


def fold2(y):
    n = y.shape[0] // 2
    return y[:n] + y[n:]


def tile_lanes(x, count):
    return jnp.concatenate([x] * count, 1)


def twice(x):
    return jnp.concatenate([x, x], 0)


def kernel(
    live_any, pos_any, kind_any, neigh_any, count_any, send_any, embed_any, site_any, win_any,
    wmid_any, wout_any, contract_any, mix_any, skip_any, rone_any, rhid_any, rout_any,
    energy_ref, forces_ref, stress_ref,
    live_ref, pos_ref, kind_ref, neigh_ref, count_ref, send_ref, embed_ref, site_ref, win_ref,
    wmid_ref, wout_ref, contract_ref, mix_ref, skip_ref, rone_ref, rhid_ref, rout_ref,
    s_ref, st_ref, oh_ref, oht_ref,
    snd1, rcv1, snd2, rcv2, snd3, rcv3, snd4, rcv4, ar1s, ar1r, ar2s, ar2r,
    rad_ref, radp_ref, feat_ref, hb_ref, a_ref, sel_ref, da_ref, gn_ref, d1_ref, d2_ref, hid_ref,
    bas_ref, basp_ref, wic_ref, wmc_ref, woc_ref, mixc_ref, mixt_ref, mixed_ref, dh_ref, q_ref,
    in_sem, ss1, rs1, ss2, rs2, ss3, rs3, ss4, rs4, sa1, ra1, sa2, ra2,
):
    arrays = [
        (pos_any, pos_ref), (kind_any, kind_ref), (send_any, send_ref), (neigh_any, neigh_ref),
        (count_any, count_ref), (live_any, live_ref), (embed_any, embed_ref), (site_any, site_ref),
        (win_any, win_ref), (wmid_any, wmid_ref), (wout_any, wout_ref), (contract_any, contract_ref),
        (mix_any, mix_ref), (skip_any, skip_ref), (rone_any, rone_ref), (rhid_any, rhid_ref),
        (rout_any, rout_ref),
    ]
    loads = [pltpu.make_async_copy(src, dst, in_sem.at[i]) for i, (src, dst) in enumerate(arrays)]
    for load in loads[:3]:
        load.start()

    p = lax.axis_index("gx")
    q = lax.axis_index("gy")
    n_gx = NX * NYH * NCORE
    n_gy = NZ * NYL

    def near(ox, oy):
        return (lax.rem(p + (ox + n_gx), n_gx), lax.rem(q + (oy + n_gy), n_gy))

    core = lax.rem(p, NCORE)
    y_hi = lax.rem(lax.div(p, NCORE), NYH)
    x = lax.div(p, NCORE * NYH)
    y_lo = lax.rem(q, NYL)
    z = lax.div(q, NYL)
    y = y_hi * NYL + y_lo

    def peer_a(i):
        yy = lax.rem(y + i // NCORE, NYH * NYL)
        cc = lax.rem(core + i % NCORE, NCORE)
        return ((x * NYH + lax.div(yy, NYL)) * NCORE + cc, z * NYL + lax.rem(yy, NYL))

    def peer_b(i):
        xx, zz = lax.rem(x + i // NZ, NX), lax.rem(z + i % NZ, NZ)
        return ((xx * NYH + y_hi) * NCORE + core, zz * NYL + y_lo)

    ahead = [near(ox, oy) for ox, oy in DIRS]
    barrier = pltpu.get_barrier_semaphore()

    def greet(who):
        pl.semaphore_signal(barrier, inc=1, device_id=who, device_id_type=pl.DeviceIdType.MESH)

    for who in ahead:
        greet(who)
    for load in loads[3:]:
        load.start()
    peers_a = [peer_a(i) for i in range(1, NYH * NYL * NCORE)]
    peers_b = [peer_b(i) for i in range(1, NX * NZ)]
    for who in peers_a + peers_b:
        greet(who)

    def remote(src, dst, ssem, rsem, who):
        return pltpu.make_async_remote_copy(
            src_ref=src, dst_ref=dst, send_sem=ssem, recv_sem=rsem, device_id=who,
            device_id_type=pl.DeviceIdType.MESH,
        )

    half = iota((8, 128), 1) < 64
    sign = 2 * core - 1

    def exchange(source, target, ssem, rsem, toward):
        outer = (1 - core) * 5 if toward < 0 else core * 5
        inner = core * 5 if toward < 0 else (1 - core) * 5
        order = [(outer + oy + 1, sign, toward * oy) for oy in (-1, 1, 0)]
        order += [(3, 0, -toward), (4, 0, toward)]
        order += [(inner + oy + 1, -sign, toward * oy) for oy in (-1, 1, 0)]
        return [
            remote(source(o), target.at[o], ssem.at[o], rsem.at[o], near(ox, oy)) for o, ox, oy in order
        ]

    for load in loads[:3]:
        load.wait()
    for b in range(4):
        row = send_ref[0:1, b * 128 : (b + 1) * 128]
        s_ref[:, b * 128 : (b + 1) * 128] = (iota((A, 128), 0) == row).astype(F32).astype(BF)
    kind = kind_ref[0:1, :]
    own8 = jnp.concatenate([pos_ref[...], kind.astype(F32), jnp.zeros((4, A), F32)], 0)
    own32 = rows3(own8)
    packet = fold3(dot(own32, s_ref[...]))
    for b in range(4):
        snd1[b] = packet[:, b * 128 : (b + 1) * 128]

    pl.semaphore_wait(barrier, len(ahead) + len(peers_a) + len(peers_b))
    copies1 = exchange(lambda o: snd1.at[lax.div(o, 2)], rcv1, ss1, rs1, -1)
    for copy in copies1:
        copy.start()

    for load in loads[3:]:
        load.wait()
    for k in range(K):
        row = neigh_ref[k : k + 1, :]
        oh_ref[:, k * A : (k + 1) * A] = (iota((A + G, A), 0) == row).astype(F32).astype(BF)
    unit = eye(128)
    for k in range(K):
        for b in range(5):
            block = oh_ref[b * 128 : (b + 1) * 128, k * A : (k + 1) * A]
            oht_ref[k * A : (k + 1) * A, b * 128 : (b + 1) * 128] = dot_tn(block, unit).astype(BF)
    for b in range(4):
        st_ref[b * 128 : (b + 1) * 128, :] = dot_tn(s_ref[:, b * 128 : (b + 1) * 128], unit).astype(BF)

    kinds4 = iota((16, A), 0)
    onehot16 = ((lax.rem(kinds4, 4) == kind) & (kinds4 < 12)).astype(F32).astype(BF)
    for l in range(2):
        in_h = win_ref[l].astype(BF).astype(F32)
        in_rows = jnp.concatenate([in_h, in_h, win_ref[l] - in_h, jnp.zeros_like(in_h)], 0)
        wic_ref[l] = dot_tn(in_rows.astype(BF), eye(32)).astype(BF)
        wmc_ref[l] = spread3(wmid_ref[l])
        oh_t, ol_t = split2(wout_ref[l])
        woc_ref[l] = dot_tn(jnp.concatenate([oh_t, oh_t, ol_t], 0), eye(3 * H)).astype(BF)
        parts = []
        for path in range(6):
            hi, mid, lo = split3(contract_ref[l, path])
            parts.append(jnp.concatenate([hi, mid, lo, jnp.zeros_like(hi)], 0).astype(BF))
        sel_ref[l] = dot_tn(jnp.concatenate(parts, 1), onehot16)
    mixh, mixl = split2(mix_ref[0])
    mixc_ref[...] = jnp.concatenate([mixh, mixh, mixl], 1)
    mth, mtl = transpose2(mix_ref[0])
    mixt_ref[...] = jnp.concatenate([mth, mth, mtl], 1)
    eh, em, el = split3(embed_ref[...])
    embed_rows = jnp.concatenate([eh, em, el, jnp.zeros_like(eh)], 0).astype(BF)
    embed16 = dot_tn(embed_rows, eye(16)).astype(BF)
    start_own = dot(embed16, onehot16)
    skip_start = dot3(skip_ref[0], start_own)
    read_mix = dot3(rhid_ref[...], mix_ref[1])
    read_skip = dot3(rhid_ref[...], skip_ref[1])
    rm_h, rm_l = split2(read_mix)
    rmc = jnp.concatenate([rm_h, rm_h, rm_l], 1)
    rmt = dot_tn(jnp.concatenate([rm_h, rm_h, rm_l], 0), eye(48)).astype(BF)
    rout = jnp.sum(jnp.where(iota((16, 16), 0) == iota((16, 16), 1), rout_ref[...], 0.0), axis=1, keepdims=True)
    live_row = (iota((1, A), 1) < live_ref[...]).astype(F32)
    site_row = jnp.zeros((1, A), F32)
    for s in range(4):
        site_row = jnp.where(kind == s, site_ref[0:1, s : s + 1], site_row)

    gathered = fold3(dot(own32, oh_ref[0:A, :]))
    for copy in copies1:
        copy.wait()
    blocks = []
    rows8 = iota((8, 128), 0)
    for b in range(4):
        (ax, ay), (bx, by) = DIRS[2 * b], DIRS[2 * b + 1]
        shift_x = jnp.where(half, float(ax), float(bx))
        shift_y = jnp.where(half, float(ay), float(by))
        shift = jnp.where(rows8 == 0, shift_x, jnp.where(rows8 == 1, shift_y, 0.0))
        blocks.append(jnp.where(half, rcv1[2 * b], rcv1[2 * b + 1]) + shift)
    ghosts8 = jnp.concatenate(blocks, 1)
    gathered = gathered + fold3(dot(rows3(ghosts8), oh_ref[A:, :]))
    own_base = jnp.where(rows8 < 3, own8, 0.0)
    edge = gathered - tile_lanes(own_base, K)
    ex, ey, ez = edge[0:1], edge[1:2], edge[2:3]
    spec_row = edge[3:4]
    scaled = (ex * ex + ey * ey + ez * ez) * 0.25
    valid = jnp.concatenate([(k < count_ref[0:1, :]).astype(F32) for k in range(K)], 1)
    cut = jnp.exp(-scaled) * valid * 0.125
    offset = (scaled - iota((8, E), 0).astype(F32) * SPACING) / SPACING
    basis = jnp.exp(-0.5 * (offset * offset))
    slope = basis * (offset * (-1.0 / SPACING))
    bh = basis.astype(BF).astype(F32)
    bas_ref[...] = jnp.concatenate([bh, basis - bh, bh, jnp.zeros_like(bh)], 0).astype(BF)
    bh = slope.astype(BF).astype(F32)
    basp_ref[...] = jnp.concatenate([bh, slope - bh, bh, jnp.zeros_like(bh)], 0).astype(BF)

    def radial(l):
        pre = dot(wic_ref[l], bas_ref[...])
        sig = jax.nn.sigmoid(pre)
        act = pre * sig
        d1_ref[l] = sig + act * (1.0 - sig)
        pre = dot(wmc_ref[l], stack3(act))
        sig = jax.nn.sigmoid(pre)
        act = pre * sig
        d2_ref[l] = sig + act * (1.0 - sig)
        hid_ref[l] = act
        rad_ref[l] = dot(woc_ref[l], stack3(act * cut))

    def radial_slopes(l):
        act = dot(wic_ref[l], basp_ref[...]) * d1_ref[l]
        act = dot(wmc_ref[l], stack3(act)) * d2_ref[l]
        radp_ref[l] = dot(woc_ref[l], stack3((act - hid_ref[l]) * cut))

    radial(0)
    kinds_e = iota((16, E), 0)
    onehot_e = ((lax.rem(kinds_e, 4).astype(F32) == spec_row) & (kinds_e < 12)).astype(F32).astype(BF)
    feat_ref[0] = dot(embed16, onehot_e)
    harmonics = [
        ex, ey, ez, ex * ey, ey * ez, ex * ez, 0.5 * (ex * ex - ey * ey),
        (2.0 * ez * ez - ex * ex - ey * ey) / 6.0,
    ]
    for m in range(8):
        hb_ref[m * 8 : (m + 1) * 8, :] = jnp.broadcast_to(harmonics[m], (8, E))

    def harm(m, at):
        return twice(hb_ref[m * 8 : (m + 1) * 8, at])

    def moments(l):
        def body(block, carry):
            c0 = pl.multiple_of(block * 16, 16)
            total = None
            for k in range(K):
                at = slice(k * A, (k + 1) * A)
                h = feat_ref[l, pl.ds(c0, 16), at]
                w0 = rad_ref[l, pl.ds(c0, 16), at] * h
                w1 = rad_ref[l, pl.ds(C + c0, 16), at] * h
                w2 = rad_ref[l, pl.ds(2 * C + c0, 16), at] * h
                terms = [w0]
                terms += [w1 * harm(m, at) for m in range(3)]
                terms += [w2 * harm(m, at) for m in range(3, 8)]
                total = terms if total is None else [t + u for t, u in zip(total, terms)]
            for m in range(9):
                a_ref[l, pl.ds(m * C + c0, 16), :] = total[m]
            a0, x1, y1, z1, xy, yz, xz, u, w = total
            q1 = x1 * x1 + y1 * y1 + z1 * z1
            q2 = xy * xy + yz * yz + xz * xz + u * u + w * w
            triple = (u - w) * (x1 * x1) - (u + w) * (y1 * y1) + 2.0 * w * (z1 * z1)
            triple = triple + 2.0 * (xy * (x1 * y1) + yz * (y1 * z1) + xz * (x1 * z1))
            s = [sel_ref[l, pl.ds(path * C + c0, 16), :] for path in range(6)]
            mixed = s[0] * a0 + s[1] * (a0 * a0) + s[2] * q1 + s[3] * q2 + s[4] * (a0 * q1) + s[5] * triple
            hi, lo = split2(mixed)
            mixed_ref[pl.ds(c0, 16), :] = hi
            mixed_ref[pl.ds(C + c0, 16), :] = lo
            mixed_ref[pl.ds(2 * C + c0, 16), :] = hi
            return carry

        lax.fori_loop(0, C // 16, body, 0)

    def moment_grads(l, block, dm):
        c0 = pl.multiple_of(block * 16, 16)
        a0, x1, y1, z1, xy, yz, xz, u, w = [a_ref[l, pl.ds(m * C + c0, 16), :] for m in range(9)]
        g = [dm * sel_ref[l, pl.ds(path * C + c0, 16), :] for path in range(6)]
        q1 = x1 * x1 + y1 * y1 + z1 * z1
        g5 = 2.0 * g[5]
        dq = 2.0 * (g[2] + a0 * g[4])
        g3 = 2.0 * g[3]
        return [
            g[0] + 2.0 * (a0 * g[1]) + q1 * g[4],
            x1 * dq + g5 * ((u - w) * x1 + xy * y1 + xz * z1),
            y1 * dq + g5 * (xy * x1 - (u + w) * y1 + yz * z1),
            z1 * dq + g5 * (xz * x1 + yz * y1 + 2.0 * (w * z1)),
            xy * g3 + g5 * (x1 * y1),
            yz * g3 + g5 * (y1 * z1),
            xz * g3 + g5 * (x1 * z1),
            u * g3 + g[5] * (x1 * x1 - y1 * y1),
            w * g3 + g[5] * (2.0 * (z1 * z1) - x1 * x1 - y1 * y1),
        ]

    def weight_grads(d, at):
        w1 = d[1] * harm(0, at) + d[2] * harm(1, at) + d[3] * harm(2, at)
        w2 = d[4] * harm(3, at) + d[5] * harm(4, at) + d[6] * harm(5, at)
        return d[0], w1, w2 + (d[7] * harm(6, at) + d[8] * harm(7, at))

    def radial_grads(l):
        def body(k, carry):
            at = pl.ds(pl.multiple_of(k * A, A), A)
            hs = [harm(m, at) for m in range(8)]
            acc = [jnp.zeros((16, A), F32)] * 9
            for block in range(C // 16):
                c0 = block * 16
                d = [da_ref[m * C + c0 : m * C + c0 + 16, :] for m in range(9)]
                h = feat_ref[l, c0 : c0 + 16, at]
                w1 = rad_ref[l, C + c0 : C + c0 + 16, at] * h
                w2 = rad_ref[l, 2 * C + c0 : 2 * C + c0 + 16, at] * h
                e1 = d[1] * hs[0] + d[2] * hs[1] + d[3] * hs[2]
                e2 = d[4] * hs[3] + d[5] * hs[4] + d[6] * hs[5] + (d[7] * hs[6] + d[8] * hs[7])
                ds = d[0] * radp_ref[l, c0 : c0 + 16, at] + e1 * radp_ref[l, C + c0 : C + c0 + 16, at]
                ds = ds + e2 * radp_ref[l, 2 * C + c0 : 2 * C + c0 + 16, at]
                acc = [acc[m] + (w1 if m < 3 else w2) * d[m + 1] for m in range(8)] + [acc[8] + ds * h]
            for m in range(9):
                dh_ref[m : m + 1, at] = jnp.sum(acc[m], axis=0, keepdims=True)
            return carry

        lax.fori_loop(0, K, body, 0)
        g0, g1, g2, g3, g4, g5, g6, g7, ds = [dh_ref[m : m + 1, :] for m in range(9)]
        ds = ds * 0.5
        third = g7 * (1.0 / 3.0)
        gx = g0 + ey * g3 + ez * g5 + ex * (g6 - third + ds)
        gy = g1 + ex * g3 + ez * g4 + ey * (ds - g6 - third)
        gz = g2 + ey * g4 + ex * g5 + ez * (2.0 * third + ds)
        return jnp.concatenate([gx, gy, gz, jnp.zeros((5, E), F32)], 0)

    moments(0)
    first = dot(mixc_ref[...], mixed_ref[...]) + skip_start

    first_h, first_l = split2(first)
    first2 = jnp.concatenate([first_h, first_l], 0)
    lane64 = iota((64, 128), 1) < 64

    def pack(value, buf):
        for b in range(4):
            top = value[0:64, b * 128 : (b + 1) * 128]
            low = value[64:128, b * 128 : (b + 1) * 128]
            buf[2 * b] = jnp.where(lane64, top, pltpu.roll(low, 64, 1))
            buf[2 * b + 1] = jnp.where(lane64, pltpu.roll(top, 64, 1), low)

    def unpack(buf, b):
        one, two = buf[2 * b], buf[2 * b + 1]
        top = jnp.where(lane64, one, pltpu.roll(two, 64, 1))
        low = jnp.where(lane64, pltpu.roll(one, 64, 1), two)
        return jnp.concatenate([top, low], 0)

    def unpack_all(buf):
        return jnp.concatenate([unpack(buf, b) for b in range(4)], 1)

    pack(fold2(dot(first2, s_ref[...])), snd2)
    copies2 = exchange(lambda o: snd2.at[o], rcv2, ss2, rs2, -1)
    for copy in copies2:
        copy.start()

    radial(1)
    radial_slopes(0)

    def strain_body(block, carry):
        c0 = pl.multiple_of(block * 16, 16)
        j0, jx, jy, jz, jxy, jyz, jxz, ju, jw = moment_grads(0, block, 1.0)
        third = jw * (1.0 / 3.0)
        mxx, myy, mzz = ju - third, -ju - third, 2.0 * third
        total = None
        for k in range(K):
            at = slice(k * A, (k + 1) * A)
            vx, vy, vz = harm(0, at), harm(1, at), harm(2, at)
            h = feat_ref[0, pl.ds(c0, 16), at]
            e1 = jx * vx + jy * vy + jz * vz
            tx = mxx * vx + jxy * vy + jxz * vz
            ty = jxy * vx + myy * vy + jyz * vz
            tz = jxz * vx + jyz * vy + mzz * vz
            e2 = 0.5 * (tx * vx + ty * vy + tz * vz)
            u = j0 * radp_ref[0, pl.ds(c0, 16), at] + e1 * radp_ref[0, pl.ds(C + c0, 16), at]
            u = (u + e2 * radp_ref[0, pl.ds(2 * C + c0, 16), at]) * (0.5 * h)
            r1 = rad_ref[0, pl.ds(C + c0, 16), at] * h
            r2 = rad_ref[0, pl.ds(2 * C + c0, 16), at] * h
            gx = vx * u + r1 * jx + r2 * tx
            gy = vy * u + r1 * jy + r2 * ty
            gz = vz * u + r1 * jz + r2 * tz
            terms = [v * g for v in (vx, vy, vz) for g in (gx, gy, gz)]
            total = terms if total is None else [t + n for t, n in zip(total, terms)]
        for n in range(9):
            q_ref[pl.ds(n * C + c0, 16), :] = total[n]
        return carry

    lax.fori_loop(0, C // 16, strain_body, 0)
    radial_slopes(1)
    feat_ref[1] = fold2(dot(first2, oh_ref[0:A, :]))
    read_base = dot3(read_skip, first)
    energy_row = live_row * (dot3(rone_ref[...], first) + site_row)

    for copy in copies2:
        copy.wait()
    gh, gl = split2(unpack_all(rcv2))
    feat_ref[1] += fold2(dot(jnp.concatenate([gh, gl], 0), oh_ref[A:, :]))

    moments(1)
    pre = dot(rmc, mixed_ref[...]) + read_base
    sig = jax.nn.sigmoid(pre)
    act = pre * sig
    energy_row = energy_row + live_row * jnp.sum(rout * act, axis=0, keepdims=True)
    dpre = rout * live_row * (sig + act * (1.0 - sig))
    dps = stack3(dpre)
    da_ref[9 * C :, :] = dot(rmt, dps)

    def neigh_body(block, carry):
        c0 = pl.multiple_of(block * 16, 16)
        d = moment_grads(1, block, da_ref[pl.ds(9 * C + c0, 16), :])
        for m in range(9):
            da_ref[pl.ds(m * C + c0, 16), :] = d[m]
        for k in range(K):
            at = slice(k * A, (k + 1) * A)
            w0, w1, w2 = weight_grads(d, at)
            g = w0 * rad_ref[1, pl.ds(c0, 16), at]
            g = g + w1 * rad_ref[1, pl.ds(C + c0, 16), at]
            g = g + w2 * rad_ref[1, pl.ds(2 * C + c0, 16), at]
            hi, lo = split2(g)
            gn_ref[pl.ds(c0, 16), at] = hi
            gn_ref[pl.ds(C + c0, 16), at] = lo
        return carry

    lax.fori_loop(0, C // 16, neigh_body, 0)
    pack(fold2(dot(gn_ref[...], oht_ref[:, A:])), snd3)
    copies3 = exchange(lambda o: snd3.at[o], rcv3, ss3, rs3, 1)
    for copy in copies3:
        copy.start()

    own_grad = fold2(dot(gn_ref[...], oht_ref[:, 0:A]))
    rs_h, rs_l = split2(read_skip)
    own_grad = own_grad + dot_tn(jnp.concatenate([rs_h, rs_h, rs_l], 0), dps)
    o_h, o_m, o_l = split3(jnp.concatenate([rone_ref[...], jnp.zeros((7, C), F32)], 0))
    live8 = jnp.where(rows8 == 0, live_row, 0.0).astype(BF)
    own_grad = own_grad + dot_tn(o_h.astype(BF), live8)
    own_grad = own_grad + (dot_tn(o_m.astype(BF), live8) + dot_tn(o_l.astype(BF), live8))
    grad_two = radial_grads(1)
    dm_own = dot(mixt_ref[...], stack3(own_grad))
    rows16, lanes16 = iota((16, 128), 0), iota((16, 128), 1)
    partial = []
    for a in range(3):
        for b in range(3):
            prod = edge[a : a + 1] * grad_two[b : b + 1]
            part = prod[:, 0:A]
            for k in range(1, K):
                part = part + prod[:, k * A : (k + 1) * A]
            partial.append(part)
    partial = jnp.concatenate(partial + [energy_row, live_row, jnp.zeros((5, A), F32)], 0)

    for copy in copies3:
        copy.wait()
    rh, rl = split2(unpack_all(rcv3))
    returned = fold2(dot(jnp.concatenate([rh, rl], 0), st_ref[...]))
    dmixed = dot(mixt_ref[...], stack3(returned)) + dm_own
    da_ref[9 * C :, :] = dmixed
    for n in range(9):
        part = jnp.sum(dmixed * q_ref[n * C : (n + 1) * C, :], axis=0, keepdims=True)
        partial = partial + jnp.where(rows16 == n, part, 0.0)
    sums = jnp.sum(partial, axis=1, keepdims=True)
    total = jnp.sum(jnp.where(lanes16 == rows16, sums, 0.0), axis=0, keepdims=True)
    ar1s[...] = total

    def spread(src, dst, ssem, rsem, peers):
        copies = [remote(src, dst.at[pl.ds(i, 1)], ssem.at[i], rsem.at[i], who) for i, who in enumerate(peers)]
        for copy in copies:
            copy.start()
        return copies

    def gather_sum(base, buf, copies):
        for copy in copies:
            copy.wait()
        count = len(copies)
        rows = buf[...]
        rows = jnp.where(iota(rows.shape, 0) < count, rows, 0.0)
        return base + jnp.sum(rows, axis=0, keepdims=True)

    reduce1 = spread(ar1s, ar1r, sa1, ra1, peers_a)

    def first_body(block, carry):
        c0 = pl.multiple_of(block * 16, 16)
        d = moment_grads(0, block, da_ref[pl.ds(9 * C + c0, 16), :])
        for m in range(9):
            da_ref[pl.ds(m * C + c0, 16), :] = d[m]
        return carry

    lax.fori_loop(0, C // 16, first_body, 0)
    grad = radial_grads(0) + grad_two

    g32 = rows3(grad)
    ghost_pos = fold3(dot(g32, oht_ref[:, A:]))
    for b in range(4):
        snd4[b] = ghost_pos[:, b * 128 : (b + 1) * 128]
    copies4 = exchange(lambda o: snd4.at[lax.div(o, 2)], rcv4, ss4, rs4, 1)
    for copy in copies4:
        copy.start()
    own_pos = fold3(dot(g32, oht_ref[:, 0:A]))
    for k in range(K):
        own_pos = own_pos - grad[:, k * A : (k + 1) * A]

    total = gather_sum(total, ar1r, reduce1)
    ar2s[...] = total
    reduce2 = spread(ar2s, ar2r, sa2, ra2, peers_b)

    for copy in copies4:
        copy.wait()
    home = jnp.concatenate([jnp.where(half, rcv4[2 * b], rcv4[2 * b + 1]) for b in range(4)], 1)
    own_pos = own_pos + fold3(dot(rows3(home), st_ref[...]))
    forces_ref[...] = -own_pos[0:3]

    total = gather_sum(total, ar2r, reduce2)
    total = total / total[:, 10:11]
    energy_ref[...] = total[:, 9:10]
    stress_ref[...] = jnp.concatenate([total[:, 0:3], total[:, 3:6], total[:, 6:9]], 0)


def per_device(
    positions, species, neighbours, counts, live_atoms, ghost_send, embed, site_energy, radial_in,
    radial_mid, radial_out, contract, mix, skip, read_one, read_hidden, read_out,
):
    vmem = pl.BlockSpec(memory_space=pltpu.VMEM)
    dma = pltpu.SemaphoreType.DMA
    operands = (
        live_atoms.reshape(1, 1), positions, species.reshape(1, A), neighbours, counts.reshape(1, A),
        ghost_send.reshape(1, G), embed.T, site_energy.reshape(1, 4), radial_in.transpose(0, 2, 1),
        radial_mid, radial_out.transpose(0, 2, 1), contract.transpose(0, 2, 1, 3), mix, skip,
        read_one.reshape(1, C), read_hidden, read_out.reshape(1, 16),
    )
    energy, forces, stress = pl.pallas_call(
        kernel,
        out_shape=(
            jax.ShapeDtypeStruct((1, 1), F32),
            jax.ShapeDtypeStruct((3, A), F32),
            jax.ShapeDtypeStruct((3, 3), F32),
        ),
        in_specs=[pl.BlockSpec(memory_space=pl.ANY)] * 17,
        out_specs=(vmem, vmem, vmem),
        scratch_shapes=[pltpu.VMEM(value.shape, value.dtype) for value in operands]
        + [
            pltpu.VMEM((A, G), BF),
            pltpu.VMEM((G, A), BF),
            pltpu.VMEM((A + G, E), BF),
            pltpu.VMEM((E, A + G), BF),
            pltpu.VMEM((4, 8, 128), F32),
            pltpu.VMEM((8, 8, 128), F32),
            pltpu.VMEM((8, 64, 128), F32),
            pltpu.VMEM((8, 64, 128), F32),
            pltpu.VMEM((8, 64, 128), F32),
            pltpu.VMEM((8, 64, 128), F32),
            pltpu.VMEM((4, 8, 128), F32),
            pltpu.VMEM((8, 8, 128), F32),
            pltpu.VMEM((1, 128), F32),
            pltpu.VMEM((16, 128), F32),
            pltpu.VMEM((1, 128), F32),
            pltpu.VMEM((32, 128), F32),
            pltpu.VMEM((2, 3 * C, E), F32),
            pltpu.VMEM((2, 3 * C, E), F32),
            pltpu.VMEM((2, C, E), F32),
            pltpu.VMEM((64, E), F32),
            pltpu.VMEM((2, 9 * C, A), F32),
            pltpu.VMEM((2, 6 * C, A), F32),
            pltpu.VMEM((10 * C, A), F32),
            pltpu.VMEM((2 * C, E), BF),
            pltpu.VMEM((2, H, E), F32),
            pltpu.VMEM((2, H, E), F32),
            pltpu.VMEM((2, H, E), F32),
            pltpu.VMEM((32, E), BF),
            pltpu.VMEM((32, E), BF),
            pltpu.VMEM((2, H, 32), BF),
            pltpu.VMEM((2, H, 3 * H), BF),
            pltpu.VMEM((2, 3 * C, 3 * H), BF),
            pltpu.VMEM((C, 3 * C), BF),
            pltpu.VMEM((C, 3 * C), BF),
            pltpu.VMEM((3 * C, A), BF),
            pltpu.VMEM((16, E), F32),
            pltpu.VMEM((9 * C, A), F32),
            dma((17,)),
            dma((8,)), dma((8,)), dma((8,)), dma((8,)), dma((8,)), dma((8,)), dma((8,)), dma((8,)),
            dma((15,)), dma((15,)), dma((31,)), dma((31,)),
        ],
        compiler_params=pltpu.CompilerParams(
            collective_id=0, has_side_effects=True, vmem_limit_bytes=56 * 1024 * 1024
        ),
    )(*operands)
    return energy.reshape(()), forces, stress


def solution(mesh):
    both = ("gx", "gy")
    placed = (P(None, both), P(both), P(None, both), P(both), P(both), P(both)) + (P(),) * 11
    return jax.shard_map(
        per_device, mesh=mesh, in_specs=placed, out_specs=(P(), P(None, both), P()), check_vma=False
    )
```

```python
import functools

import jax
import jax.numpy as jnp
from jax import lax
from jax.experimental import pallas as pl
from jax.experimental.pallas import tpu as pltpu
from jax.sharding import PartitionSpec as P

F32 = jnp.float32
BF = jnp.bfloat16
C = 128
H = 64
K = 8
A = 128
E = K * A
G = 512
DIRS = ((-1, -1), (-1, 0), (-1, 1), (0, -1), (0, 1), (1, -1), (1, 0), (1, 1))
NX, NYH, NCORE = 4, 4, 2
NZ, NYL = 8, 2
SPACING = 2.0 / 7.0


def dot(a, b):
    return lax.dot_general(a, b, (((1,), (0,)), ((), ())), preferred_element_type=F32)


def dot_nt(a, b):
    return lax.dot_general(a, b, (((1,), (1,)), ((), ())), preferred_element_type=F32)


def dot_tn(a, b):
    return lax.dot_general(a, b, (((0,), (0,)), ((), ())), preferred_element_type=F32)


def split2(x):
    hi = x.astype(BF)
    return hi, (x - hi.astype(F32)).astype(BF)


def split3(x):
    hi = x.astype(BF).astype(F32)
    rest = x - hi
    mid = rest.astype(BF).astype(F32)
    return hi, mid, rest - mid


def dot3(a, b):
    ah, al = split2(a)
    bh, bl = split2(b)
    return dot(ah, bh) + (dot(ah, bl) + dot(al, bh))


def stack3(x):
    hi, lo = split2(x)
    return jnp.concatenate([hi, lo, hi], 0)


def iota(shape, axis):
    return lax.broadcasted_iota(jnp.int32, shape, axis)


def eye(n, dtype=BF):
    return (iota((n, n), 0) == iota((n, n), 1)).astype(F32).astype(dtype)


def spread3(w):
    n = w.shape[1]
    hi, lo = split2(w)
    row, col = iota((n, 3 * n), 0), iota((n, 3 * n), 1)
    first = ((col == row) | (col == row + n)).astype(F32).astype(BF)
    last = (col == row + 2 * n).astype(F32).astype(BF)
    return (dot(hi, first) + dot(lo, last)).astype(BF)


def transpose2(w):
    hi, lo = split2(w)
    unit = eye(w.shape[1])
    return dot_nt(unit, hi).astype(BF), dot_nt(unit, lo).astype(BF)


def rows3(x):
    hi, mid, lo = split3(x)
    return jnp.concatenate([hi, mid, lo, jnp.zeros_like(hi)], 0).astype(BF)


def fold3(y):
    return y[0:8] + (y[8:16] + y[16:24])


def fold2(y):
    n = y.shape[0] // 2
    return y[:n] + y[n:]


def tile_lanes(x, count):
    return jnp.concatenate([x] * count, 1)


def lanes_at(x, index):
    return jnp.take_along_axis(x, index, axis=1, mode="promise_in_bounds")


def twice(x):
    return jnp.concatenate([x, x], 0)


def kernel(
    live_any, pos_any, kind_any, neigh_any, count_any, send_any, embed_any, site_any, win_any,
    wmid_any, wout_any, contract_any, mix_any, skip_any, rone_any, rhid_any, rout_any,
    out_ref,
    live_ref, pos_ref, kind_ref, neigh_ref, count_ref, send_ref, embed_ref, site_ref, win_ref,
    wmid_ref, wout_ref, contract_ref, mix_ref, skip_ref, rone_ref, rhid_ref, rout_ref,
    s_ref, st_ref, oh_ref, oht_ref,
    snd1, rcv1, snd2, rcv2, snd3, rcv3, snd4, rcv4, ar1s, ar1r, ar2s, ar2r,
    rad_ref, radp_ref, feat_ref, hb_ref, a_ref, sel_ref, da_ref, gn_ref, d1_ref, d2_ref, hid_ref,
    bas_ref, basp_ref, wic_ref, wmc_ref, woc_ref, mixc_ref, mixt_ref, mixed_ref, dh_ref, q_ref,
    in_sem, ss1, rs1, ss2, rs2, ss3, rs3, ss4, rs4, sa1, ra1, sa2, ra2,
):
    arrays = [
        (pos_any, pos_ref), (kind_any, kind_ref), (send_any, send_ref), (neigh_any, neigh_ref),
        (count_any, count_ref), (live_any, live_ref), (embed_any, embed_ref), (site_any, site_ref),
        (win_any, win_ref), (wmid_any, wmid_ref), (wout_any, wout_ref), (contract_any, contract_ref),
        (mix_any, mix_ref), (skip_any, skip_ref), (rone_any, rone_ref), (rhid_any, rhid_ref),
        (rout_any, rout_ref),
    ]
    loads = [pltpu.make_async_copy(src, dst, in_sem.at[i]) for i, (src, dst) in enumerate(arrays)]
    for load in loads[:3]:
        load.start()

    p = lax.axis_index("gx")
    q = lax.axis_index("gy")
    n_gx = NX * NYH * NCORE
    n_gy = NZ * NYL

    def near(ox, oy):
        return (lax.rem(p + (ox + n_gx), n_gx), lax.rem(q + (oy + n_gy), n_gy))

    core = lax.rem(p, NCORE)
    y_hi = lax.rem(lax.div(p, NCORE), NYH)
    x = lax.div(p, NCORE * NYH)
    y_lo = lax.rem(q, NYL)
    z = lax.div(q, NYL)
    y = y_hi * NYL + y_lo

    def peer_a(i):
        yy = lax.rem(y + i // NCORE, NYH * NYL)
        cc = lax.rem(core + i % NCORE, NCORE)
        return ((x * NYH + lax.div(yy, NYL)) * NCORE + cc, z * NYL + lax.rem(yy, NYL))

    def peer_b(i):
        xx, zz = lax.rem(x + i // NZ, NX), lax.rem(z + i % NZ, NZ)
        return ((xx * NYH + y_hi) * NCORE + core, zz * NYL + y_lo)

    ahead = [near(ox, oy) for ox, oy in DIRS]
    barrier = pltpu.get_barrier_semaphore()

    def greet(who):
        pl.semaphore_signal(barrier, inc=1, device_id=who, device_id_type=pl.DeviceIdType.MESH)

    for who in ahead:
        greet(who)
    for load in loads[3:]:
        load.start()
    def ring(i, n):
        return min(i, n - i)

    far_a = lambda i: (-ring(i // NCORE, NYH * NYL), i)
    far_b = lambda i: (-ring(i // NZ, NX) - ring(i % NZ, NZ), i)
    peers_a = [peer_a(i) for i in sorted(range(1, NYH * NYL * NCORE), key=far_a)]
    peers_b = [peer_b(i) for i in sorted(range(1, NX * NZ), key=far_b)]
    for who in peers_a + peers_b:
        greet(who)

    def remote(src, dst, ssem, rsem, who):
        return pltpu.make_async_remote_copy(
            src_ref=src, dst_ref=dst, send_sem=ssem, recv_sem=rsem, device_id=who,
            device_id_type=pl.DeviceIdType.MESH,
        )

    half = iota((8, 128), 1) < 64
    sign = 2 * core - 1

    def exchange(source, target, ssem, rsem, toward):
        outer = (1 - core) * 5 if toward < 0 else core * 5
        inner = core * 5 if toward < 0 else (1 - core) * 5
        order = [(outer + oy + 1, sign, toward * oy) for oy in (-1, 1, 0)]
        order += [(3, 0, -toward), (4, 0, toward)]
        order += [(inner + oy + 1, -sign, toward * oy) for oy in (-1, 1, 0)]
        return [
            remote(source(o), target.at[o], ssem.at[o], rsem.at[o], near(ox, oy)) for o, ox, oy in order
        ]

    for load in loads[:3]:
        load.wait()
    for b in range(4):
        row = send_ref[0:1, b * 128 : (b + 1) * 128]
        s_ref[:, b * 128 : (b + 1) * 128] = (iota((A, 128), 0) == row).astype(F32).astype(BF)
    kind = kind_ref[0:1, :]
    own8 = jnp.concatenate([pos_ref[...], kind.astype(F32), jnp.zeros((4, A), F32)], 0)
    own32 = rows3(own8)
    packet = fold3(dot(own32, s_ref[...]))
    for b in range(4):
        snd1[b] = packet[:, b * 128 : (b + 1) * 128]

    pl.semaphore_wait(barrier, len(ahead) + len(peers_a) + len(peers_b))
    copies1 = exchange(lambda o: snd1.at[lax.div(o, 2)], rcv1, ss1, rs1, -1)
    for copy in copies1:
        copy.start()

    for load in loads[3:]:
        load.wait()
    for k in range(K):
        row = neigh_ref[k : k + 1, :]
        oh_ref[:, k * A : (k + 1) * A] = (iota((A + G, A), 0) == row).astype(F32).astype(BF)
    unit = eye(128)
    for k in range(K):
        for b in range(5):
            block = oh_ref[b * 128 : (b + 1) * 128, k * A : (k + 1) * A]
            oht_ref[k * A : (k + 1) * A, b * 128 : (b + 1) * 128] = dot_tn(block, unit).astype(BF)
    for b in range(4):
        st_ref[b * 128 : (b + 1) * 128, :] = dot_tn(s_ref[:, b * 128 : (b + 1) * 128], unit).astype(BF)

    kinds4 = iota((16, A), 0)
    onehot16 = ((lax.rem(kinds4, 4) == kind) & (kinds4 < 12)).astype(F32).astype(BF)
    for l in range(2):
        in_h = win_ref[l].astype(BF).astype(F32)
        in_rows = jnp.concatenate([in_h, in_h, win_ref[l] - in_h, jnp.zeros_like(in_h)], 0)
        wic_ref[l] = dot_tn(in_rows.astype(BF), eye(32)).astype(BF)
        wmc_ref[l] = spread3(wmid_ref[l])
        oh_t, ol_t = split2(wout_ref[l])
        woc_ref[l] = dot_tn(jnp.concatenate([oh_t, oh_t, ol_t], 0), eye(3 * H)).astype(BF)
        parts = []
        for path in range(6):
            hi, mid, lo = split3(contract_ref[l, path])
            parts.append(jnp.concatenate([hi, mid, lo, jnp.zeros_like(hi)], 0).astype(BF))
        sel_ref[l] = dot_tn(jnp.concatenate(parts, 1), onehot16)
    mixh, mixl = split2(mix_ref[0])
    mixc_ref[...] = jnp.concatenate([mixh, mixh, mixl], 1)
    mth, mtl = transpose2(mix_ref[0])
    mixt_ref[...] = jnp.concatenate([mth, mth, mtl], 1)
    eh, em, el = split3(embed_ref[...])
    embed_rows = jnp.concatenate([eh, em, el, jnp.zeros_like(eh)], 0).astype(BF)
    embed16 = dot_tn(embed_rows, eye(16)).astype(BF)
    start_own = dot(embed16, onehot16)
    skip_start = dot3(skip_ref[0], start_own)
    read_mix = dot3(rhid_ref[...], mix_ref[1])
    read_skip = dot3(rhid_ref[...], skip_ref[1])
    rm_h, rm_l = split2(read_mix)
    rmc = jnp.concatenate([rm_h, rm_h, rm_l], 1)
    rmt = dot_tn(jnp.concatenate([rm_h, rm_h, rm_l], 0), eye(48)).astype(BF)
    rout = jnp.sum(jnp.where(iota((16, 16), 0) == iota((16, 16), 1), rout_ref[...], 0.0), axis=1, keepdims=True)
    live_row = (iota((1, A), 1) < live_ref[0]).astype(F32)
    site_row = jnp.zeros((1, A), F32)
    for s in range(4):
        site_row = jnp.where(kind == s, site_ref[0:1, s : s + 1], site_row)

    for copy in copies1:
        copy.wait()
    blocks = []
    rows8 = iota((8, 128), 0)
    for b in range(4):
        (ax, ay), (bx, by) = DIRS[2 * b], DIRS[2 * b + 1]
        shift_x = jnp.where(half, float(ax), float(bx))
        shift_y = jnp.where(half, float(ay), float(by))
        shift = jnp.where(rows8 == 0, shift_x, jnp.where(rows8 == 1, shift_y, 0.0))
        blocks.append(jnp.where(half, rcv1[2 * b], rcv1[2 * b + 1]) + shift)
    gathered = []
    for k in range(K):
        index = jnp.broadcast_to(neigh_ref[k : k + 1, :], (8, 128))
        place_in, lane = lax.shift_right_logical(index, 7), lax.bitwise_and(index, 127)
        picked = lanes_at(own8, lane)
        for b in range(4):
            picked = jnp.where(place_in == b + 1, lanes_at(blocks[b], lane), picked)
        gathered.append(picked)
    gathered = jnp.concatenate(gathered, 1)
    own_base = jnp.where(rows8 < 3, own8, 0.0)
    edge = gathered - tile_lanes(own_base, K)
    ex, ey, ez = edge[0:1], edge[1:2], edge[2:3]
    spec_row = edge[3:4]
    scaled = (ex * ex + ey * ey + ez * ez) * 0.25
    valid = jnp.concatenate([(k < count_ref[0:1, :]).astype(F32) for k in range(K)], 1)
    cut = jnp.exp(-scaled) * valid * 0.125
    offset = (scaled - iota((8, E), 0).astype(F32) * SPACING) / SPACING
    basis = jnp.exp(-0.5 * (offset * offset))
    slope = basis * (offset * (-1.0 / SPACING))
    bh = basis.astype(BF).astype(F32)
    bas_ref[...] = jnp.concatenate([bh, basis - bh, bh, jnp.zeros_like(bh)], 0).astype(BF)
    bh = slope.astype(BF).astype(F32)
    basp_ref[...] = jnp.concatenate([bh, slope - bh, bh, jnp.zeros_like(bh)], 0).astype(BF)

    def radial(l):
        pre = dot(wic_ref[l], bas_ref[...])
        sig = jax.nn.sigmoid(pre)
        act = pre * sig
        d1_ref[l] = sig + act * (1.0 - sig)
        pre = dot(wmc_ref[l], stack3(act))
        sig = jax.nn.sigmoid(pre)
        act = pre * sig
        d2_ref[l] = sig + act * (1.0 - sig)
        hid_ref[l] = act
        rad_ref[l] = dot(woc_ref[l], stack3(act * cut))

    def radial_slopes(l):
        act = dot(wic_ref[l], basp_ref[...]) * d1_ref[l]
        act = dot(wmc_ref[l], stack3(act)) * d2_ref[l]
        radp_ref[l] = dot(woc_ref[l], stack3((act - hid_ref[l]) * cut))

    radial(0)
    kinds_e = iota((16, E), 0)
    onehot_e = ((lax.rem(kinds_e, 4).astype(F32) == spec_row) & (kinds_e < 12)).astype(F32).astype(BF)
    feat_ref[0] = dot(embed16, onehot_e)
    harmonics = [
        ex, ey, ez, ex * ey, ey * ez, ex * ez, 0.5 * (ex * ex - ey * ey),
        (2.0 * ez * ez - ex * ex - ey * ey) / 6.0,
    ]
    for m in range(8):
        hb_ref[m * 8 : (m + 1) * 8, :] = jnp.broadcast_to(harmonics[m], (8, E))

    def harm(m, at):
        return twice(hb_ref[m * 8 : (m + 1) * 8, at])

    def moments(l):
        def body(block, carry):
            c0 = pl.multiple_of(block * 16, 16)
            total = None
            for k in range(K):
                at = slice(k * A, (k + 1) * A)
                h = feat_ref[l, pl.ds(c0, 16), at]
                w0 = rad_ref[l, pl.ds(c0, 16), at] * h
                w1 = rad_ref[l, pl.ds(C + c0, 16), at] * h
                w2 = rad_ref[l, pl.ds(2 * C + c0, 16), at] * h
                terms = [w0]
                terms += [w1 * harm(m, at) for m in range(3)]
                terms += [w2 * harm(m, at) for m in range(3, 8)]
                total = terms if total is None else [t + u for t, u in zip(total, terms)]
            for m in range(9):
                a_ref[l, pl.ds(m * C + c0, 16), :] = total[m]
            a0, x1, y1, z1, xy, yz, xz, u, w = total
            q1 = x1 * x1 + y1 * y1 + z1 * z1
            q2 = xy * xy + yz * yz + xz * xz + u * u + w * w
            triple = (u - w) * (x1 * x1) - (u + w) * (y1 * y1) + 2.0 * w * (z1 * z1)
            triple = triple + 2.0 * (xy * (x1 * y1) + yz * (y1 * z1) + xz * (x1 * z1))
            s = [sel_ref[l, pl.ds(path * C + c0, 16), :] for path in range(6)]
            mixed = s[0] * a0 + s[1] * (a0 * a0) + s[2] * q1 + s[3] * q2 + s[4] * (a0 * q1) + s[5] * triple
            hi, lo = split2(mixed)
            mixed_ref[pl.ds(c0, 16), :] = hi
            mixed_ref[pl.ds(C + c0, 16), :] = lo
            mixed_ref[pl.ds(2 * C + c0, 16), :] = hi
            return carry

        lax.fori_loop(0, C // 16, body, 0)

    def moment_grads(l, block, dm):
        c0 = pl.multiple_of(block * 16, 16)
        a0, x1, y1, z1, xy, yz, xz, u, w = [a_ref[l, pl.ds(m * C + c0, 16), :] for m in range(9)]
        g = [dm * sel_ref[l, pl.ds(path * C + c0, 16), :] for path in range(6)]
        q1 = x1 * x1 + y1 * y1 + z1 * z1
        g5 = 2.0 * g[5]
        dq = 2.0 * (g[2] + a0 * g[4])
        g3 = 2.0 * g[3]
        return [
            g[0] + 2.0 * (a0 * g[1]) + q1 * g[4],
            x1 * dq + g5 * ((u - w) * x1 + xy * y1 + xz * z1),
            y1 * dq + g5 * (xy * x1 - (u + w) * y1 + yz * z1),
            z1 * dq + g5 * (xz * x1 + yz * y1 + 2.0 * (w * z1)),
            xy * g3 + g5 * (x1 * y1),
            yz * g3 + g5 * (y1 * z1),
            xz * g3 + g5 * (x1 * z1),
            u * g3 + g[5] * (x1 * x1 - y1 * y1),
            w * g3 + g[5] * (2.0 * (z1 * z1) - x1 * x1 - y1 * y1),
        ]

    def weight_grads(d, at):
        w1 = d[1] * harm(0, at) + d[2] * harm(1, at) + d[3] * harm(2, at)
        w2 = d[4] * harm(3, at) + d[5] * harm(4, at) + d[6] * harm(5, at)
        return d[0], w1, w2 + (d[7] * harm(6, at) + d[8] * harm(7, at))

    def radial_grads(l):
        def body(k, carry):
            at = pl.ds(pl.multiple_of(k * A, A), A)
            hs = [harm(m, at) for m in range(8)]
            acc = [jnp.zeros((16, A), F32)] * 9
            for block in range(C // 16):
                c0 = block * 16
                d = [da_ref[m * C + c0 : m * C + c0 + 16, :] for m in range(9)]
                h = feat_ref[l, c0 : c0 + 16, at]
                w1 = rad_ref[l, C + c0 : C + c0 + 16, at] * h
                w2 = rad_ref[l, 2 * C + c0 : 2 * C + c0 + 16, at] * h
                e1 = d[1] * hs[0] + d[2] * hs[1] + d[3] * hs[2]
                e2 = d[4] * hs[3] + d[5] * hs[4] + d[6] * hs[5] + (d[7] * hs[6] + d[8] * hs[7])
                ds = d[0] * radp_ref[l, c0 : c0 + 16, at] + e1 * radp_ref[l, C + c0 : C + c0 + 16, at]
                ds = ds + e2 * radp_ref[l, 2 * C + c0 : 2 * C + c0 + 16, at]
                acc = [acc[m] + (w1 if m < 3 else w2) * d[m + 1] for m in range(8)] + [acc[8] + ds * h]
            for m in range(9):
                dh_ref[m : m + 1, at] = jnp.sum(acc[m], axis=0, keepdims=True)
            return carry

        lax.fori_loop(0, K, body, 0)
        g0, g1, g2, g3, g4, g5, g6, g7, ds = [dh_ref[m : m + 1, :] for m in range(9)]
        ds = ds * 0.5
        third = g7 * (1.0 / 3.0)
        gx = g0 + ey * g3 + ez * g5 + ex * (g6 - third + ds)
        gy = g1 + ex * g3 + ez * g4 + ey * (ds - g6 - third)
        gz = g2 + ey * g4 + ex * g5 + ez * (2.0 * third + ds)
        return jnp.concatenate([gx, gy, gz, jnp.zeros((5, E), F32)], 0)

    moments(0)
    first = dot(mixc_ref[...], mixed_ref[...]) + skip_start

    first_h, first_l = split2(first)
    first2 = jnp.concatenate([first_h, first_l], 0)
    lane64 = iota((64, 128), 1) < 64

    def pack(value, buf):
        for b in range(4):
            top = value[0:64, b * 128 : (b + 1) * 128]
            low = value[64:128, b * 128 : (b + 1) * 128]
            buf[2 * b] = jnp.where(lane64, top, pltpu.roll(low, 64, 1))
            buf[2 * b + 1] = jnp.where(lane64, pltpu.roll(top, 64, 1), low)

    def unpack(buf, b):
        one, two = buf[2 * b], buf[2 * b + 1]
        top = jnp.where(lane64, one, pltpu.roll(two, 64, 1))
        low = jnp.where(lane64, pltpu.roll(one, 64, 1), two)
        return jnp.concatenate([top, low], 0)

    def unpack_all(buf):
        return jnp.concatenate([unpack(buf, b) for b in range(4)], 1)

    pack(fold2(dot(first2, s_ref[...])), snd2)
    copies2 = exchange(lambda o: snd2.at[o], rcv2, ss2, rs2, -1)
    for copy in copies2:
        copy.start()

    radial(1)
    radial_slopes(0)

    def strain_body(block, carry):
        c0 = pl.multiple_of(block * 16, 16)
        j0, jx, jy, jz, jxy, jyz, jxz, ju, jw = moment_grads(0, block, 1.0)
        third = jw * (1.0 / 3.0)
        mxx, myy, mzz = ju - third, -ju - third, 2.0 * third
        total = None
        for k in range(K):
            at = slice(k * A, (k + 1) * A)
            vx, vy, vz = harm(0, at), harm(1, at), harm(2, at)
            h = feat_ref[0, pl.ds(c0, 16), at]
            e1 = jx * vx + jy * vy + jz * vz
            tx = mxx * vx + jxy * vy + jxz * vz
            ty = jxy * vx + myy * vy + jyz * vz
            tz = jxz * vx + jyz * vy + mzz * vz
            e2 = 0.5 * (tx * vx + ty * vy + tz * vz)
            u = j0 * radp_ref[0, pl.ds(c0, 16), at] + e1 * radp_ref[0, pl.ds(C + c0, 16), at]
            u = (u + e2 * radp_ref[0, pl.ds(2 * C + c0, 16), at]) * (0.5 * h)
            r1 = rad_ref[0, pl.ds(C + c0, 16), at] * h
            r2 = rad_ref[0, pl.ds(2 * C + c0, 16), at] * h
            gx = vx * u + r1 * jx + r2 * tx
            gy = vy * u + r1 * jy + r2 * ty
            gz = vz * u + r1 * jz + r2 * tz
            terms = [v * g for v in (vx, vy, vz) for g in (gx, gy, gz)]
            total = terms if total is None else [t + n for t, n in zip(total, terms)]
        for n in range(9):
            q_ref[pl.ds(n * C + c0, 16), :] = total[n]
        return carry

    lax.fori_loop(0, C // 16, strain_body, 0)
    radial_slopes(1)
    feat_ref[1] = fold2(dot(first2, oh_ref[0:A, :]))
    read_base = dot3(read_skip, first)
    energy_row = live_row * (dot3(rone_ref[...], first) + site_row)

    for copy in copies2:
        copy.wait()
    gh, gl = split2(unpack_all(rcv2))
    feat_ref[1] += fold2(dot(jnp.concatenate([gh, gl], 0), oh_ref[A:, :]))

    moments(1)
    pre = dot(rmc, mixed_ref[...]) + read_base
    sig = jax.nn.sigmoid(pre)
    act = pre * sig
    energy_row = energy_row + live_row * jnp.sum(rout * act, axis=0, keepdims=True)
    dpre = rout * live_row * (sig + act * (1.0 - sig))
    dps = stack3(dpre)
    da_ref[9 * C :, :] = dot(rmt, dps)

    def neigh_body(block, carry):
        c0 = pl.multiple_of(block * 16, 16)
        d = moment_grads(1, block, da_ref[pl.ds(9 * C + c0, 16), :])
        for m in range(9):
            da_ref[pl.ds(m * C + c0, 16), :] = d[m]
        for k in range(K):
            at = slice(k * A, (k + 1) * A)
            w0, w1, w2 = weight_grads(d, at)
            g = w0 * rad_ref[1, pl.ds(c0, 16), at]
            g = g + w1 * rad_ref[1, pl.ds(C + c0, 16), at]
            g = g + w2 * rad_ref[1, pl.ds(2 * C + c0, 16), at]
            hi, lo = split2(g)
            gn_ref[pl.ds(c0, 16), at] = hi
            gn_ref[pl.ds(C + c0, 16), at] = lo
        return carry

    lax.fori_loop(0, C // 16, neigh_body, 0)
    pack(fold2(dot(gn_ref[...], oht_ref[:, A:])), snd3)
    copies3 = exchange(lambda o: snd3.at[o], rcv3, ss3, rs3, 1)
    for copy in copies3:
        copy.start()

    own_grad = fold2(dot(gn_ref[...], oht_ref[:, 0:A]))
    rs_h, rs_l = split2(read_skip)
    own_grad = own_grad + dot_tn(jnp.concatenate([rs_h, rs_h, rs_l], 0), dps)
    o_h, o_m, o_l = split3(jnp.concatenate([rone_ref[...], jnp.zeros((7, C), F32)], 0))
    live8 = jnp.where(rows8 == 0, live_row, 0.0).astype(BF)
    own_grad = own_grad + dot_tn(o_h.astype(BF), live8)
    own_grad = own_grad + (dot_tn(o_m.astype(BF), live8) + dot_tn(o_l.astype(BF), live8))
    grad_two = radial_grads(1)
    dm_own = dot(mixt_ref[...], stack3(own_grad))
    rows16, lanes16 = iota((16, 128), 0), iota((16, 128), 1)
    partial = []
    for a in range(3):
        for b in range(3):
            prod = edge[a : a + 1] * grad_two[b : b + 1]
            part = prod[:, 0:A]
            for k in range(1, K):
                part = part + prod[:, k * A : (k + 1) * A]
            partial.append(part)
    partial = jnp.concatenate(partial + [energy_row, live_row, jnp.zeros((5, A), F32)], 0)

    for copy in copies3:
        copy.wait()
    rh, rl = split2(unpack_all(rcv3))
    returned = fold2(dot(jnp.concatenate([rh, rl], 0), st_ref[...]))
    dmixed = dot(mixt_ref[...], stack3(returned)) + dm_own
    da_ref[9 * C :, :] = dmixed
    for n in range(9):
        part = jnp.sum(dmixed * q_ref[n * C : (n + 1) * C, :], axis=0, keepdims=True)
        partial = partial + jnp.where(rows16 == n, part, 0.0)
    sums = jnp.sum(partial, axis=1, keepdims=True)
    total = jnp.sum(jnp.where(lanes16 == rows16, sums, 0.0), axis=0, keepdims=True)
    ar1s[...] = total

    def spread(src, dst, ssem, rsem, peers):
        copies = [remote(src, dst.at[pl.ds(i, 1)], ssem.at[i], rsem.at[i], who) for i, who in enumerate(peers)]
        for copy in copies:
            copy.start()
        return copies

    def gather_sum(base, buf, copies):
        for copy in copies:
            copy.wait()
        count = len(copies)
        rows = buf[...]
        rows = jnp.where(iota(rows.shape, 0) < count, rows, 0.0)
        return base + jnp.sum(rows, axis=0, keepdims=True)

    reduce1 = spread(ar1s, ar1r, sa1, ra1, peers_a)

    def first_body(block, carry):
        c0 = pl.multiple_of(block * 16, 16)
        d = moment_grads(0, block, da_ref[pl.ds(9 * C + c0, 16), :])
        for m in range(9):
            da_ref[pl.ds(m * C + c0, 16), :] = d[m]
        return carry

    lax.fori_loop(0, C // 16, first_body, 0)
    grad = radial_grads(0) + grad_two

    g32 = rows3(grad)
    ghost_pos = fold3(dot(g32, oht_ref[:, A:]))
    for b in range(4):
        snd4[b] = ghost_pos[:, b * 128 : (b + 1) * 128]
    copies4 = exchange(lambda o: snd4.at[lax.div(o, 2)], rcv4, ss4, rs4, 1)
    for copy in copies4:
        copy.start()
    own_pos = fold3(dot(g32, oht_ref[:, 0:A]))
    for k in range(K):
        own_pos = own_pos - grad[:, k * A : (k + 1) * A]

    total = gather_sum(total, ar1r, reduce1)
    ar2s[...] = total
    reduce2 = spread(ar2s, ar2r, sa2, ra2, peers_b)

    for copy in copies4:
        copy.wait()
    home = jnp.concatenate([jnp.where(half, rcv4[2 * b], rcv4[2 * b + 1]) for b in range(4)], 1)
    own_pos = own_pos + fold3(dot(rows3(home), st_ref[...]))
    out_ref[0:3, :] = -own_pos[0:3]

    total = gather_sum(total, ar2r, reduce2)
    total = total / total[:, 10:11]
    out_ref[3:4, :] = total


def finish(out_ref, energy_ref, forces_ref, stress_ref):
    forces_ref[...] = out_ref[0:3, :]
    total = out_ref[3:4, :]
    energy_ref[...] = total[:, 9:10]
    stress_ref[...] = jnp.concatenate([total[:, 0:3], total[:, 3:6], total[:, 6:9]], 0)


def per_device(
    positions, species, neighbours, counts, live_atoms, ghost_send, embed, site_energy, radial_in,
    radial_mid, radial_out, contract, mix, skip, read_one, read_hidden, read_out,
):
    vmem = pl.BlockSpec(memory_space=pltpu.VMEM)
    dma = pltpu.SemaphoreType.DMA
    operands = (
        live_atoms, positions, species.reshape(1, A), neighbours, counts.reshape(1, A),
        ghost_send.reshape(1, G), embed.T, site_energy.reshape(1, 4), radial_in.transpose(0, 2, 1),
        radial_mid, radial_out.transpose(0, 2, 1), contract.transpose(0, 2, 1, 3), mix, skip,
        read_one.reshape(1, C), read_hidden, read_out.reshape(1, 16),
    )
    result = pl.pallas_call(
        kernel,
        out_shape=pltpu.VMEM((8, A), F32),
        in_specs=[pl.BlockSpec(memory_space=pl.ANY)] * 17,
        out_specs=vmem,
        scratch_shapes=[pltpu.SMEM((1,), jnp.int32)]
        + [pltpu.VMEM(value.shape, value.dtype) for value in operands[1:]]
        + [
            pltpu.VMEM((A, G), BF),
            pltpu.VMEM((G, A), BF),
            pltpu.VMEM((A + G, E), BF),
            pltpu.VMEM((E, A + G), BF),
            pltpu.VMEM((4, 8, 128), F32),
            pltpu.VMEM((8, 8, 128), F32),
            pltpu.VMEM((8, 64, 128), F32),
            pltpu.VMEM((8, 64, 128), F32),
            pltpu.VMEM((8, 64, 128), F32),
            pltpu.VMEM((8, 64, 128), F32),
            pltpu.VMEM((4, 8, 128), F32),
            pltpu.VMEM((8, 8, 128), F32),
            pltpu.VMEM((1, 128), F32),
            pltpu.VMEM((16, 128), F32),
            pltpu.VMEM((1, 128), F32),
            pltpu.VMEM((32, 128), F32),
            pltpu.VMEM((2, 3 * C, E), F32),
            pltpu.VMEM((2, 3 * C, E), F32),
            pltpu.VMEM((2, C, E), F32),
            pltpu.VMEM((64, E), F32),
            pltpu.VMEM((2, 9 * C, A), F32),
            pltpu.VMEM((2, 6 * C, A), F32),
            pltpu.VMEM((10 * C, A), F32),
            pltpu.VMEM((2 * C, E), BF),
            pltpu.VMEM((2, H, E), F32),
            pltpu.VMEM((2, H, E), F32),
            pltpu.VMEM((2, H, E), F32),
            pltpu.VMEM((32, E), BF),
            pltpu.VMEM((32, E), BF),
            pltpu.VMEM((2, H, 32), BF),
            pltpu.VMEM((2, H, 3 * H), BF),
            pltpu.VMEM((2, 3 * C, 3 * H), BF),
            pltpu.VMEM((C, 3 * C), BF),
            pltpu.VMEM((C, 3 * C), BF),
            pltpu.VMEM((3 * C, A), BF),
            pltpu.VMEM((16, E), F32),
            pltpu.VMEM((9 * C, A), F32),
            dma((17,)),
            dma((8,)), dma((8,)), dma((8,)), dma((8,)), dma((8,)), dma((8,)), dma((8,)), dma((8,)),
            dma((15,)), dma((15,)), dma((31,)), dma((31,)),
        ],
        compiler_params=pltpu.CompilerParams(
            collective_id=0, has_side_effects=True, vmem_limit_bytes=56 * 1024 * 1024
        ),
    )(*operands)
    energy, forces, stress = pl.pallas_call(
        finish,
        out_shape=(
            jax.ShapeDtypeStruct((1, 1), F32),
            jax.ShapeDtypeStruct((3, A), F32),
            jax.ShapeDtypeStruct((3, 3), F32),
        ),
        in_specs=[vmem],
        out_specs=(vmem, vmem, vmem),
    )(pltpu.with_memory_space_constraint(result, pltpu.VMEM))
    return energy.reshape(()), forces, stress


def solution(mesh):
    both = ("gx", "gy")
    placed = (P(None, both), P(both), P(None, both), P(both), P(both), P(both)) + (P(),) * 11
    return jax.shard_map(
        per_device, mesh=mesh, in_specs=placed, out_specs=(P(), P(None, both), P()), check_vma=False
    )
```

```python
import functools

import jax
import jax.numpy as jnp
from jax import lax
from jax.experimental import pallas as pl
from jax.experimental.pallas import tpu as pltpu
from jax.sharding import PartitionSpec as P

F32 = jnp.float32
BF = jnp.bfloat16
C = 128
H = 64
K = 8
A = 128
E = K * A
G = 512
DIRS = ((-1, -1), (-1, 0), (-1, 1), (0, -1), (0, 1), (1, -1), (1, 0), (1, 1))
NX, NYH, NCORE = 4, 4, 2
NZ, NYL = 8, 2
SPACING = 2.0 / 7.0


def dot(a, b):
    return lax.dot_general(a, b, (((1,), (0,)), ((), ())), preferred_element_type=F32)


def dot_nt(a, b):
    return lax.dot_general(a, b, (((1,), (1,)), ((), ())), preferred_element_type=F32)


def dot_tn(a, b):
    return lax.dot_general(a, b, (((0,), (0,)), ((), ())), preferred_element_type=F32)


def split2(x):
    hi = x.astype(BF)
    return hi, (x - hi.astype(F32)).astype(BF)


def split3(x):
    hi = x.astype(BF).astype(F32)
    rest = x - hi
    mid = rest.astype(BF).astype(F32)
    return hi, mid, rest - mid


def dot3(a, b):
    ah, al = split2(a)
    bh, bl = split2(b)
    return dot(ah, bh) + (dot(ah, bl) + dot(al, bh))


def stack3(x):
    hi, lo = split2(x)
    return jnp.concatenate([hi, lo, hi], 0)


def iota(shape, axis):
    return lax.broadcasted_iota(jnp.int32, shape, axis)


def eye(n, dtype=BF):
    return (iota((n, n), 0) == iota((n, n), 1)).astype(F32).astype(dtype)


def spread3(w):
    n = w.shape[1]
    hi, lo = split2(w)
    row, col = iota((n, 3 * n), 0), iota((n, 3 * n), 1)
    first = ((col == row) | (col == row + n)).astype(F32).astype(BF)
    last = (col == row + 2 * n).astype(F32).astype(BF)
    return (dot(hi, first) + dot(lo, last)).astype(BF)


def transpose2(w):
    hi, lo = split2(w)
    unit = eye(w.shape[1])
    return dot_nt(unit, hi).astype(BF), dot_nt(unit, lo).astype(BF)


def rows3(x):
    hi, mid, lo = split3(x)
    return jnp.concatenate([hi, mid, lo, jnp.zeros_like(hi)], 0).astype(BF)


def fold3(y):
    return y[0:8] + (y[8:16] + y[16:24])


def fold2(y):
    n = y.shape[0] // 2
    return y[:n] + y[n:]


def tile_lanes(x, count):
    return jnp.concatenate([x] * count, 1)


def lanes_at(x, index):
    return jnp.take_along_axis(x, index, axis=1, mode="promise_in_bounds")


def twice(x):
    return jnp.concatenate([x, x], 0)


def kernel(
    live_any, pos_any, kind_any, neigh_any, count_any, send_any, embed_any, site_any, win_any,
    wmid_any, wout_any, contract_any, mix_any, skip_any, rone_any, rhid_any, rout_any,
    out_ref,
    live_ref, pos_ref, kind_ref, neigh_ref, count_ref, send_ref, embed_ref, site_ref, win_ref,
    wmid_ref, wout_ref, contract_ref, mix_ref, skip_ref, rone_ref, rhid_ref, rout_ref,
    s_ref, st_ref, oh_ref, oht_ref,
    snd1, rcv1, snd2, rcv2, snd3, rcv3, snd4, rcv4, ar1s, ar1r, ar2s, ar2r,
    rad_ref, radp_ref, feat_ref, hb_ref, a_ref, sel_ref, da_ref, gn_ref, d1_ref, d2_ref, hid_ref,
    bas_ref, basp_ref, wic_ref, wmc_ref, woc_ref, mixc_ref, mixt_ref, mixed_ref, dh_ref, q_ref,
    in_sem, ss1, rs1, ss2, rs2, ss3, rs3, ss4, rs4, sa1, ra1, sa2, ra2,
):
    arrays = [
        (pos_any, pos_ref), (kind_any, kind_ref), (send_any, send_ref), (neigh_any, neigh_ref),
        (count_any, count_ref), (live_any, live_ref), (embed_any, embed_ref), (site_any, site_ref),
        (win_any, win_ref), (wmid_any, wmid_ref), (wout_any, wout_ref), (contract_any, contract_ref),
        (mix_any, mix_ref), (skip_any, skip_ref), (rone_any, rone_ref), (rhid_any, rhid_ref),
        (rout_any, rout_ref),
    ]
    loads = [pltpu.make_async_copy(src, dst, in_sem.at[i]) for i, (src, dst) in enumerate(arrays)]
    for load in loads[:3]:
        load.start()

    p = lax.axis_index("gx")
    q = lax.axis_index("gy")
    n_gx = NX * NYH * NCORE
    n_gy = NZ * NYL

    def near(ox, oy):
        return (lax.rem(p + (ox + n_gx), n_gx), lax.rem(q + (oy + n_gy), n_gy))

    core = lax.rem(p, NCORE)
    y_hi = lax.rem(lax.div(p, NCORE), NYH)
    x = lax.div(p, NCORE * NYH)
    y_lo = lax.rem(q, NYL)
    z = lax.div(q, NYL)
    y = y_hi * NYL + y_lo

    def peer_a(i):
        yy = lax.rem(y + i // NCORE, NYH * NYL)
        cc = lax.rem(core + i % NCORE, NCORE)
        return ((x * NYH + lax.div(yy, NYL)) * NCORE + cc, z * NYL + lax.rem(yy, NYL))

    def peer_b(i):
        xx, zz = lax.rem(x + i // NZ, NX), lax.rem(z + i % NZ, NZ)
        return ((xx * NYH + y_hi) * NCORE + core, zz * NYL + y_lo)

    ahead = [near(ox, oy) for ox, oy in DIRS]
    barrier = pltpu.get_barrier_semaphore()

    def greet(who):
        pl.semaphore_signal(barrier, inc=1, device_id=who, device_id_type=pl.DeviceIdType.MESH)

    for who in ahead:
        greet(who)
    for load in loads[3:]:
        load.start()
    def ring(i, n):
        return min(i, n - i)

    far_a = lambda i: (-ring(i // NCORE, NYH * NYL), i)
    far_b = lambda i: (-ring(i // NZ, NX) - ring(i % NZ, NZ), i)
    peers_a = [peer_a(i) for i in sorted(range(1, NYH * NYL * NCORE), key=far_a)]
    peers_b = [peer_b(i) for i in sorted(range(1, NX * NZ), key=far_b)]
    for who in peers_a + peers_b:
        greet(who)

    def remote(src, dst, ssem, rsem, who):
        return pltpu.make_async_remote_copy(
            src_ref=src, dst_ref=dst, send_sem=ssem, recv_sem=rsem, device_id=who,
            device_id_type=pl.DeviceIdType.MESH,
        )

    half = iota((8, 128), 1) < 64
    sign = 2 * core - 1

    def arrive(source, target, ssem, rsem, first_slot):
        for i in range(4):
            o = first_slot + i
            remote(source.at[o], target.at[o], ssem.at[o], rsem.at[o], ahead[0]).wait_recv()

    def exchange(source, target, ssem, rsem, toward):
        outer = (1 - core) * 5 if toward < 0 else core * 5
        inner = core * 5 if toward < 0 else (1 - core) * 5
        order = [(outer + oy + 1, sign, toward * oy) for oy in (-1, 1, 0)]
        order += [(3, 0, -toward), (4, 0, toward)]
        order += [(inner + oy + 1, -sign, toward * oy) for oy in (-1, 1, 0)]
        return [
            remote(source(o), target.at[o], ssem.at[o], rsem.at[o], near(ox, oy)) for o, ox, oy in order
        ]

    for load in loads[:3]:
        load.wait()
    for b in range(4):
        row = send_ref[0:1, b * 128 : (b + 1) * 128]
        s_ref[:, b * 128 : (b + 1) * 128] = (iota((A, 128), 0) == row).astype(F32).astype(BF)
    kind = kind_ref[0:1, :]
    own8 = jnp.concatenate([pos_ref[...], kind.astype(F32), jnp.zeros((4, A), F32)], 0)
    own32 = rows3(own8)
    packet = fold3(dot(own32, s_ref[...]))
    for b in range(4):
        snd1[b] = packet[:, b * 128 : (b + 1) * 128]

    pl.semaphore_wait(barrier, len(ahead) + len(peers_a) + len(peers_b))
    copies1 = exchange(lambda o: snd1.at[lax.div(o, 2)], rcv1, ss1, rs1, -1)
    for copy in copies1:
        copy.start()

    for load in loads[3:]:
        load.wait()
    for k in range(K):
        row = neigh_ref[k : k + 1, :]
        oh_ref[:, k * A : (k + 1) * A] = (iota((A + G, A), 0) == row).astype(F32).astype(BF)
    unit = eye(128)
    for k in range(K):
        for b in range(5):
            block = oh_ref[b * 128 : (b + 1) * 128, k * A : (k + 1) * A]
            oht_ref[k * A : (k + 1) * A, b * 128 : (b + 1) * 128] = dot_tn(block, unit).astype(BF)
    for b in range(4):
        st_ref[b * 128 : (b + 1) * 128, :] = dot_tn(s_ref[:, b * 128 : (b + 1) * 128], unit).astype(BF)

    kinds4 = iota((16, A), 0)
    onehot16 = ((lax.rem(kinds4, 4) == kind) & (kinds4 < 12)).astype(F32).astype(BF)
    for l in range(2):
        in_h = win_ref[l].astype(BF).astype(F32)
        in_rows = jnp.concatenate([in_h, in_h, win_ref[l] - in_h, jnp.zeros_like(in_h)], 0)
        wic_ref[l] = dot_tn(in_rows.astype(BF), eye(32)).astype(BF)
        wmc_ref[l] = spread3(wmid_ref[l])
        oh_t, ol_t = split2(wout_ref[l])
        woc_ref[l] = dot_tn(jnp.concatenate([oh_t, oh_t, ol_t], 0), eye(3 * H)).astype(BF)
        parts = []
        for path in range(6):
            hi, mid, lo = split3(contract_ref[l, path])
            parts.append(jnp.concatenate([hi, mid, lo, jnp.zeros_like(hi)], 0).astype(BF))
        sel_ref[l] = dot_tn(jnp.concatenate(parts, 1), onehot16)
    mixh, mixl = split2(mix_ref[0])
    mixc_ref[...] = jnp.concatenate([mixh, mixh, mixl], 1)
    mth, mtl = transpose2(mix_ref[0])
    mixt_ref[...] = jnp.concatenate([mth, mth, mtl], 1)
    eh, em, el = split3(embed_ref[...])
    embed_rows = jnp.concatenate([eh, em, el, jnp.zeros_like(eh)], 0).astype(BF)
    embed16 = dot_tn(embed_rows, eye(16)).astype(BF)
    start_own = dot(embed16, onehot16)
    skip_start = dot3(skip_ref[0], start_own)
    read_mix = dot3(rhid_ref[...], mix_ref[1])
    read_skip = dot3(rhid_ref[...], skip_ref[1])
    rm_h, rm_l = split2(read_mix)
    rmc = jnp.concatenate([rm_h, rm_h, rm_l], 1)
    rmt = dot_tn(jnp.concatenate([rm_h, rm_h, rm_l], 0), eye(48)).astype(BF)
    rout = jnp.sum(jnp.where(iota((16, 16), 0) == iota((16, 16), 1), rout_ref[...], 0.0), axis=1, keepdims=True)
    live_row = (iota((1, A), 1) < live_ref[0]).astype(F32)
    site_row = jnp.zeros((1, A), F32)
    for s in range(4):
        site_row = jnp.where(kind == s, site_ref[0:1, s : s + 1], site_row)

    for copy in copies1:
        copy.wait()
    blocks = []
    rows8 = iota((8, 128), 0)
    for b in range(4):
        (ax, ay), (bx, by) = DIRS[2 * b], DIRS[2 * b + 1]
        shift_x = jnp.where(half, float(ax), float(bx))
        shift_y = jnp.where(half, float(ay), float(by))
        shift = jnp.where(rows8 == 0, shift_x, jnp.where(rows8 == 1, shift_y, 0.0))
        blocks.append(jnp.where(half, rcv1[2 * b], rcv1[2 * b + 1]) + shift)
    gathered = []
    for k in range(K):
        index = jnp.broadcast_to(neigh_ref[k : k + 1, :], (8, 128))
        place_in, lane = lax.shift_right_logical(index, 7), lax.bitwise_and(index, 127)
        picked = lanes_at(own8, lane)
        for b in range(4):
            picked = jnp.where(place_in == b + 1, lanes_at(blocks[b], lane), picked)
        gathered.append(picked)
    gathered = jnp.concatenate(gathered, 1)
    own_base = jnp.where(rows8 < 3, own8, 0.0)
    edge = gathered - tile_lanes(own_base, K)
    ex, ey, ez = edge[0:1], edge[1:2], edge[2:3]
    spec_row = edge[3:4]
    scaled = (ex * ex + ey * ey + ez * ez) * 0.25
    valid = jnp.concatenate([(k < count_ref[0:1, :]).astype(F32) for k in range(K)], 1)
    cut = jnp.exp(-scaled) * valid * 0.125
    offset = (scaled - iota((8, E), 0).astype(F32) * SPACING) / SPACING
    basis = jnp.exp(-0.5 * (offset * offset))
    slope = basis * (offset * (-1.0 / SPACING))
    bh = basis.astype(BF).astype(F32)
    bas_ref[...] = jnp.concatenate([bh, basis - bh, bh, jnp.zeros_like(bh)], 0).astype(BF)
    bh = slope.astype(BF).astype(F32)
    basp_ref[...] = jnp.concatenate([bh, slope - bh, bh, jnp.zeros_like(bh)], 0).astype(BF)

    def radial(l):
        pre = dot(wic_ref[l], bas_ref[...])
        sig = jax.nn.sigmoid(pre)
        act = pre * sig
        d1_ref[l] = sig + act * (1.0 - sig)
        pre = dot(wmc_ref[l], stack3(act))
        sig = jax.nn.sigmoid(pre)
        act = pre * sig
        d2_ref[l] = sig + act * (1.0 - sig)
        hid_ref[l] = act
        rad_ref[l] = dot(woc_ref[l], stack3(act * cut))

    def radial_slopes(l):
        act = dot(wic_ref[l], basp_ref[...]) * d1_ref[l]
        act = dot(wmc_ref[l], stack3(act)) * d2_ref[l]
        radp_ref[l] = dot(woc_ref[l], stack3((act - hid_ref[l]) * cut))

    radial(0)
    kinds_e = iota((16, E), 0)
    onehot_e = ((lax.rem(kinds_e, 4).astype(F32) == spec_row) & (kinds_e < 12)).astype(F32).astype(BF)
    feat_ref[0] = dot(embed16, onehot_e)
    harmonics = [
        ex, ey, ez, ex * ey, ey * ez, ex * ez, 0.5 * (ex * ex - ey * ey),
        (2.0 * ez * ez - ex * ex - ey * ey) / 6.0,
    ]
    for m in range(8):
        hb_ref[m * 8 : (m + 1) * 8, :] = jnp.broadcast_to(harmonics[m], (8, E))

    def harm(m, at):
        return twice(hb_ref[m * 8 : (m + 1) * 8, at])

    def moments(l):
        def body(block, carry):
            c0 = pl.multiple_of(block * 16, 16)
            total = None
            for k in range(K):
                at = slice(k * A, (k + 1) * A)
                h = feat_ref[l, pl.ds(c0, 16), at]
                w0 = rad_ref[l, pl.ds(c0, 16), at] * h
                w1 = rad_ref[l, pl.ds(C + c0, 16), at] * h
                w2 = rad_ref[l, pl.ds(2 * C + c0, 16), at] * h
                terms = [w0]
                terms += [w1 * harm(m, at) for m in range(3)]
                terms += [w2 * harm(m, at) for m in range(3, 8)]
                total = terms if total is None else [t + u for t, u in zip(total, terms)]
            for m in range(9):
                a_ref[l, pl.ds(m * C + c0, 16), :] = total[m]
            a0, x1, y1, z1, xy, yz, xz, u, w = total
            q1 = x1 * x1 + y1 * y1 + z1 * z1
            q2 = xy * xy + yz * yz + xz * xz + u * u + w * w
            triple = (u - w) * (x1 * x1) - (u + w) * (y1 * y1) + 2.0 * w * (z1 * z1)
            triple = triple + 2.0 * (xy * (x1 * y1) + yz * (y1 * z1) + xz * (x1 * z1))
            s = [sel_ref[l, pl.ds(path * C + c0, 16), :] for path in range(6)]
            mixed = s[0] * a0 + s[1] * (a0 * a0) + s[2] * q1 + s[3] * q2 + s[4] * (a0 * q1) + s[5] * triple
            hi, lo = split2(mixed)
            mixed_ref[pl.ds(c0, 16), :] = hi
            mixed_ref[pl.ds(C + c0, 16), :] = lo
            mixed_ref[pl.ds(2 * C + c0, 16), :] = hi
            return carry

        lax.fori_loop(0, C // 16, body, 0)

    def moment_grads(l, block, dm):
        c0 = pl.multiple_of(block * 16, 16)
        a0, x1, y1, z1, xy, yz, xz, u, w = [a_ref[l, pl.ds(m * C + c0, 16), :] for m in range(9)]
        g = [dm * sel_ref[l, pl.ds(path * C + c0, 16), :] for path in range(6)]
        q1 = x1 * x1 + y1 * y1 + z1 * z1
        g5 = 2.0 * g[5]
        dq = 2.0 * (g[2] + a0 * g[4])
        g3 = 2.0 * g[3]
        return [
            g[0] + 2.0 * (a0 * g[1]) + q1 * g[4],
            x1 * dq + g5 * ((u - w) * x1 + xy * y1 + xz * z1),
            y1 * dq + g5 * (xy * x1 - (u + w) * y1 + yz * z1),
            z1 * dq + g5 * (xz * x1 + yz * y1 + 2.0 * (w * z1)),
            xy * g3 + g5 * (x1 * y1),
            yz * g3 + g5 * (y1 * z1),
            xz * g3 + g5 * (x1 * z1),
            u * g3 + g[5] * (x1 * x1 - y1 * y1),
            w * g3 + g[5] * (2.0 * (z1 * z1) - x1 * x1 - y1 * y1),
        ]

    def weight_grads(d, at):
        w1 = d[1] * harm(0, at) + d[2] * harm(1, at) + d[3] * harm(2, at)
        w2 = d[4] * harm(3, at) + d[5] * harm(4, at) + d[6] * harm(5, at)
        return d[0], w1, w2 + (d[7] * harm(6, at) + d[8] * harm(7, at))

    def radial_grads(l):
        def body(k, carry):
            at = pl.ds(pl.multiple_of(k * A, A), A)
            hs = [harm(m, at) for m in range(8)]
            acc = [jnp.zeros((16, A), F32)] * 9
            for block in range(C // 16):
                c0 = block * 16
                d = [da_ref[m * C + c0 : m * C + c0 + 16, :] for m in range(9)]
                h = feat_ref[l, c0 : c0 + 16, at]
                w1 = rad_ref[l, C + c0 : C + c0 + 16, at] * h
                w2 = rad_ref[l, 2 * C + c0 : 2 * C + c0 + 16, at] * h
                e1 = d[1] * hs[0] + d[2] * hs[1] + d[3] * hs[2]
                e2 = d[4] * hs[3] + d[5] * hs[4] + d[6] * hs[5] + (d[7] * hs[6] + d[8] * hs[7])
                ds = d[0] * radp_ref[l, c0 : c0 + 16, at] + e1 * radp_ref[l, C + c0 : C + c0 + 16, at]
                ds = ds + e2 * radp_ref[l, 2 * C + c0 : 2 * C + c0 + 16, at]
                acc = [acc[m] + (w1 if m < 3 else w2) * d[m + 1] for m in range(8)] + [acc[8] + ds * h]
            for m in range(9):
                dh_ref[m : m + 1, at] = jnp.sum(acc[m], axis=0, keepdims=True)
            return carry

        lax.fori_loop(0, K, body, 0)
        g0, g1, g2, g3, g4, g5, g6, g7, ds = [dh_ref[m : m + 1, :] for m in range(9)]
        ds = ds * 0.5
        third = g7 * (1.0 / 3.0)
        gx = g0 + ey * g3 + ez * g5 + ex * (g6 - third + ds)
        gy = g1 + ex * g3 + ez * g4 + ey * (ds - g6 - third)
        gz = g2 + ey * g4 + ex * g5 + ez * (2.0 * third + ds)
        return jnp.concatenate([gx, gy, gz, jnp.zeros((5, E), F32)], 0)

    moments(0)
    first = dot(mixc_ref[...], mixed_ref[...]) + skip_start

    first_h, first_l = split2(first)
    first2 = jnp.concatenate([first_h, first_l], 0)
    lane64 = iota((64, 128), 1) < 64

    def pack(value, buf):
        for b in range(4):
            top = value[0:64, b * 128 : (b + 1) * 128]
            low = value[64:128, b * 128 : (b + 1) * 128]
            buf[2 * b] = jnp.where(lane64, top, pltpu.roll(low, 64, 1))
            buf[2 * b + 1] = jnp.where(lane64, pltpu.roll(top, 64, 1), low)

    def unpack(buf, b):
        one, two = buf[2 * b], buf[2 * b + 1]
        top = jnp.where(lane64, one, pltpu.roll(two, 64, 1))
        low = jnp.where(lane64, pltpu.roll(one, 64, 1), two)
        return jnp.concatenate([top, low], 0)

    def unpack_two(buf, slot):
        return jnp.concatenate([unpack(buf, slot), unpack(buf, slot + 1)], 1)

    pack(fold2(dot(first2, s_ref[...])), snd2)
    copies2 = exchange(lambda o: snd2.at[o], rcv2, ss2, rs2, -1)
    for copy in copies2:
        copy.start()

    radial(1)
    radial_slopes(0)

    def strain_body(block, carry):
        c0 = pl.multiple_of(block * 16, 16)
        j0, jx, jy, jz, jxy, jyz, jxz, ju, jw = moment_grads(0, block, 1.0)
        third = jw * (1.0 / 3.0)
        mxx, myy, mzz = ju - third, -ju - third, 2.0 * third
        total = None
        for k in range(K):
            at = slice(k * A, (k + 1) * A)
            vx, vy, vz = harm(0, at), harm(1, at), harm(2, at)
            h = feat_ref[0, pl.ds(c0, 16), at]
            e1 = jx * vx + jy * vy + jz * vz
            tx = mxx * vx + jxy * vy + jxz * vz
            ty = jxy * vx + myy * vy + jyz * vz
            tz = jxz * vx + jyz * vy + mzz * vz
            e2 = 0.5 * (tx * vx + ty * vy + tz * vz)
            u = j0 * radp_ref[0, pl.ds(c0, 16), at] + e1 * radp_ref[0, pl.ds(C + c0, 16), at]
            u = (u + e2 * radp_ref[0, pl.ds(2 * C + c0, 16), at]) * (0.5 * h)
            r1 = rad_ref[0, pl.ds(C + c0, 16), at] * h
            r2 = rad_ref[0, pl.ds(2 * C + c0, 16), at] * h
            gx = vx * u + r1 * jx + r2 * tx
            gy = vy * u + r1 * jy + r2 * ty
            gz = vz * u + r1 * jz + r2 * tz
            terms = [v * g for v in (vx, vy, vz) for g in (gx, gy, gz)]
            total = terms if total is None else [t + n for t, n in zip(total, terms)]
        for n in range(9):
            q_ref[pl.ds(n * C + c0, 16), :] = total[n]
        return carry

    lax.fori_loop(0, C // 16, strain_body, 0)
    radial_slopes(1)
    feat_ref[1] = fold2(dot(first2, oh_ref[0:A, :]))
    read_base = dot3(read_skip, first)
    energy_row = live_row * (dot3(rone_ref[...], first) + site_row)

    for group in range(2):
        pair = (1 - core) * 2 if group == 0 else core * 2
        arrive(snd2, rcv2, ss2, rs2, 2 * pair)
        gh, gl = split2(unpack_two(rcv2, pair))
        rows = pl.ds(pl.multiple_of(A + pair * 128, 128), 256)
        feat_ref[1] += fold2(dot(jnp.concatenate([gh, gl], 0), oh_ref[rows, :]))

    moments(1)
    pre = dot(rmc, mixed_ref[...]) + read_base
    sig = jax.nn.sigmoid(pre)
    act = pre * sig
    energy_row = energy_row + live_row * jnp.sum(rout * act, axis=0, keepdims=True)
    dpre = rout * live_row * (sig + act * (1.0 - sig))
    dps = stack3(dpre)
    da_ref[9 * C :, :] = dot(rmt, dps)

    def neigh_body(block, carry):
        c0 = pl.multiple_of(block * 16, 16)
        d = moment_grads(1, block, da_ref[pl.ds(9 * C + c0, 16), :])
        for m in range(9):
            da_ref[pl.ds(m * C + c0, 16), :] = d[m]
        for k in range(K):
            at = slice(k * A, (k + 1) * A)
            w0, w1, w2 = weight_grads(d, at)
            g = w0 * rad_ref[1, pl.ds(c0, 16), at]
            g = g + w1 * rad_ref[1, pl.ds(C + c0, 16), at]
            g = g + w2 * rad_ref[1, pl.ds(2 * C + c0, 16), at]
            hi, lo = split2(g)
            gn_ref[pl.ds(c0, 16), at] = hi
            gn_ref[pl.ds(C + c0, 16), at] = lo
        return carry

    lax.fori_loop(0, C // 16, neigh_body, 0)
    pack(fold2(dot(gn_ref[...], oht_ref[:, A:])), snd3)
    copies3 = exchange(lambda o: snd3.at[o], rcv3, ss3, rs3, 1)
    for copy in copies3:
        copy.start()

    own_grad = fold2(dot(gn_ref[...], oht_ref[:, 0:A]))
    rs_h, rs_l = split2(read_skip)
    own_grad = own_grad + dot_tn(jnp.concatenate([rs_h, rs_h, rs_l], 0), dps)
    o_h, o_m, o_l = split3(jnp.concatenate([rone_ref[...], jnp.zeros((7, C), F32)], 0))
    live8 = jnp.where(rows8 == 0, live_row, 0.0).astype(BF)
    own_grad = own_grad + dot_tn(o_h.astype(BF), live8)
    own_grad = own_grad + (dot_tn(o_m.astype(BF), live8) + dot_tn(o_l.astype(BF), live8))
    grad_two = radial_grads(1)
    for n in range(3):
        at = [q_ref[(3 * n + m) * C : (3 * n + m + 1) * C, :] for m in range(3)]
        moved = dot(mixc_ref[...], stack3(jnp.concatenate(at, 1)))
        for m in range(3):
            q_ref[(3 * n + m) * C : (3 * n + m + 1) * C, :] = moved[:, m * 128 : (m + 1) * 128]
    rows16, lanes16 = iota((16, 128), 0), iota((16, 128), 1)
    partial = []
    for a in range(3):
        for b in range(3):
            prod = edge[a : a + 1] * grad_two[b : b + 1]
            part = prod[:, 0:A]
            for k in range(1, K):
                part = part + prod[:, k * A : (k + 1) * A]
            partial.append(part)
    partial = jnp.concatenate(partial + [energy_row, live_row, jnp.zeros((5, A), F32)], 0)

    returned = own_grad
    for group in range(2):
        pair = core * 2 if group == 0 else (1 - core) * 2
        arrive(snd3, rcv3, ss3, rs3, 2 * pair)
        rh, rl = split2(unpack_two(rcv3, pair))
        rows = pl.ds(pl.multiple_of(pair * 128, 128), 256)
        returned = returned + fold2(dot(jnp.concatenate([rh, rl], 0), st_ref[rows, :]))
    for n in range(9):
        part = jnp.sum(returned * q_ref[n * C : (n + 1) * C, :], axis=0, keepdims=True)
        partial = partial + jnp.where(rows16 == n, part, 0.0)
    sums = jnp.sum(partial, axis=1, keepdims=True)
    total = jnp.sum(jnp.where(lanes16 == rows16, sums, 0.0), axis=0, keepdims=True)
    ar1s[...] = total

    def spread(src, dst, ssem, rsem, peers):
        copies = [remote(src, dst.at[pl.ds(i, 1)], ssem.at[i], rsem.at[i], who) for i, who in enumerate(peers)]
        for copy in copies:
            copy.start()
        return copies

    def gather_sum(base, buf, copies):
        for copy in copies:
            copy.wait()
        count = len(copies)
        rows = buf[...]
        rows = jnp.where(iota(rows.shape, 0) < count, rows, 0.0)
        return base + jnp.sum(rows, axis=0, keepdims=True)

    reduce1 = spread(ar1s, ar1r, sa1, ra1, peers_a)
    da_ref[9 * C :, :] = dot(mixt_ref[...], stack3(returned))

    def first_body(block, carry):
        c0 = pl.multiple_of(block * 16, 16)
        d = moment_grads(0, block, da_ref[pl.ds(9 * C + c0, 16), :])
        for m in range(9):
            da_ref[pl.ds(m * C + c0, 16), :] = d[m]
        return carry

    lax.fori_loop(0, C // 16, first_body, 0)
    grad = radial_grads(0) + grad_two

    g32 = rows3(grad)
    ghost_pos = fold3(dot(g32, oht_ref[:, A:]))
    for b in range(4):
        snd4[b] = ghost_pos[:, b * 128 : (b + 1) * 128]
    copies4 = exchange(lambda o: snd4.at[lax.div(o, 2)], rcv4, ss4, rs4, 1)
    for copy in copies4:
        copy.start()
    own_pos = fold3(dot(g32, oht_ref[:, 0:A]))
    for k in range(K):
        own_pos = own_pos - grad[:, k * A : (k + 1) * A]

    total = gather_sum(total, ar1r, reduce1)
    ar2s[...] = total
    reduce2 = spread(ar2s, ar2r, sa2, ra2, peers_b)

    for copy in copies4:
        copy.wait()
    home = jnp.concatenate([jnp.where(half, rcv4[2 * b], rcv4[2 * b + 1]) for b in range(4)], 1)
    own_pos = own_pos + fold3(dot(rows3(home), st_ref[...]))
    out_ref[0:3, :] = -own_pos[0:3]

    total = gather_sum(total, ar2r, reduce2)
    total = total / total[:, 10:11]
    for copy in copies2 + copies3:
        copy.wait_send()
    out_ref[3:4, :] = total


def finish(out_ref, energy_ref, forces_ref, stress_ref):
    forces_ref[...] = out_ref[0:3, :]
    total = out_ref[3:4, :]
    energy_ref[...] = total[:, 9:10]
    stress_ref[...] = jnp.concatenate([total[:, 0:3], total[:, 3:6], total[:, 6:9]], 0)


def per_device(
    positions, species, neighbours, counts, live_atoms, ghost_send, embed, site_energy, radial_in,
    radial_mid, radial_out, contract, mix, skip, read_one, read_hidden, read_out,
):
    vmem = pl.BlockSpec(memory_space=pltpu.VMEM)
    dma = pltpu.SemaphoreType.DMA
    operands = (
        live_atoms, positions, species.reshape(1, A), neighbours, counts.reshape(1, A),
        ghost_send.reshape(1, G), embed.T, site_energy.reshape(1, 4), radial_in.transpose(0, 2, 1),
        radial_mid, radial_out.transpose(0, 2, 1), contract.transpose(0, 2, 1, 3), mix, skip,
        read_one.reshape(1, C), read_hidden, read_out.reshape(1, 16),
    )
    result = pl.pallas_call(
        kernel,
        out_shape=pltpu.VMEM((8, A), F32),
        in_specs=[pl.BlockSpec(memory_space=pl.ANY)] * 17,
        out_specs=vmem,
        scratch_shapes=[pltpu.SMEM((1,), jnp.int32)]
        + [pltpu.VMEM(value.shape, value.dtype) for value in operands[1:]]
        + [
            pltpu.VMEM((A, G), BF),
            pltpu.VMEM((G, A), BF),
            pltpu.VMEM((A + G, E), BF),
            pltpu.VMEM((E, A + G), BF),
            pltpu.VMEM((4, 8, 128), F32),
            pltpu.VMEM((8, 8, 128), F32),
            pltpu.VMEM((8, 64, 128), F32),
            pltpu.VMEM((8, 64, 128), F32),
            pltpu.VMEM((8, 64, 128), F32),
            pltpu.VMEM((8, 64, 128), F32),
            pltpu.VMEM((4, 8, 128), F32),
            pltpu.VMEM((8, 8, 128), F32),
            pltpu.VMEM((1, 128), F32),
            pltpu.VMEM((16, 128), F32),
            pltpu.VMEM((1, 128), F32),
            pltpu.VMEM((32, 128), F32),
            pltpu.VMEM((2, 3 * C, E), F32),
            pltpu.VMEM((2, 3 * C, E), F32),
            pltpu.VMEM((2, C, E), F32),
            pltpu.VMEM((64, E), F32),
            pltpu.VMEM((2, 9 * C, A), F32),
            pltpu.VMEM((2, 6 * C, A), F32),
            pltpu.VMEM((10 * C, A), F32),
            pltpu.VMEM((2 * C, E), BF),
            pltpu.VMEM((2, H, E), F32),
            pltpu.VMEM((2, H, E), F32),
            pltpu.VMEM((2, H, E), F32),
            pltpu.VMEM((32, E), BF),
            pltpu.VMEM((32, E), BF),
            pltpu.VMEM((2, H, 32), BF),
            pltpu.VMEM((2, H, 3 * H), BF),
            pltpu.VMEM((2, 3 * C, 3 * H), BF),
            pltpu.VMEM((C, 3 * C), BF),
            pltpu.VMEM((C, 3 * C), BF),
            pltpu.VMEM((3 * C, A), BF),
            pltpu.VMEM((16, E), F32),
            pltpu.VMEM((9 * C, A), F32),
            dma((17,)),
            dma((8,)), dma((8,)), dma((8,)), dma((8,)), dma((8,)), dma((8,)), dma((8,)), dma((8,)),
            dma((15,)), dma((15,)), dma((31,)), dma((31,)),
        ],
        compiler_params=pltpu.CompilerParams(
            collective_id=0, has_side_effects=True, vmem_limit_bytes=56 * 1024 * 1024
        ),
    )(*operands)
    energy, forces, stress = pl.pallas_call(
        finish,
        out_shape=(
            jax.ShapeDtypeStruct((1, 1), F32),
            jax.ShapeDtypeStruct((3, A), F32),
            jax.ShapeDtypeStruct((3, 3), F32),
        ),
        in_specs=[vmem],
        out_specs=(vmem, vmem, vmem),
    )(pltpu.with_memory_space_constraint(result, pltpu.VMEM))
    return energy.reshape(()), forces, stress


def solution(mesh):
    both = ("gx", "gy")
    placed = (P(None, both), P(both), P(None, both), P(both), P(both), P(both)) + (P(),) * 11
    return jax.shard_map(
        per_device, mesh=mesh, in_specs=placed, out_specs=(P(), P(None, both), P()), check_vma=False
    )
```

```python
import functools

import jax
import jax.numpy as jnp
from jax import lax
from jax.experimental import pallas as pl
from jax.experimental.pallas import tpu as pltpu
from jax.sharding import PartitionSpec as P

F32 = jnp.float32
BF = jnp.bfloat16
C = 128
H = 64
K = 8
A = 128
E = K * A
G = 512
DIRS = ((-1, -1), (-1, 0), (-1, 1), (0, -1), (0, 1), (1, -1), (1, 0), (1, 1))
NX, NYH, NCORE = 4, 4, 2
NZ, NYL = 8, 2
SPACING = 2.0 / 7.0


def dot(a, b):
    return lax.dot_general(a, b, (((1,), (0,)), ((), ())), preferred_element_type=F32)


def dot_nt(a, b):
    return lax.dot_general(a, b, (((1,), (1,)), ((), ())), preferred_element_type=F32)


def dot_tn(a, b):
    return lax.dot_general(a, b, (((0,), (0,)), ((), ())), preferred_element_type=F32)


def split2(x):
    hi = x.astype(BF)
    return hi, (x - hi.astype(F32)).astype(BF)


def split3(x):
    hi = x.astype(BF).astype(F32)
    rest = x - hi
    mid = rest.astype(BF).astype(F32)
    return hi, mid, rest - mid


def dot3(a, b):
    ah, al = split2(a)
    bh, bl = split2(b)
    return dot(ah, bh) + (dot(ah, bl) + dot(al, bh))


def stack3(x):
    hi, lo = split2(x)
    return jnp.concatenate([hi, lo, hi], 0)


def iota(shape, axis):
    return lax.broadcasted_iota(jnp.int32, shape, axis)


def eye(n, dtype=BF):
    return (iota((n, n), 0) == iota((n, n), 1)).astype(F32).astype(dtype)


def spread3(w):
    n = w.shape[1]
    hi, lo = split2(w)
    row, col = iota((n, 3 * n), 0), iota((n, 3 * n), 1)
    first = ((col == row) | (col == row + n)).astype(F32).astype(BF)
    last = (col == row + 2 * n).astype(F32).astype(BF)
    return (dot(hi, first) + dot(lo, last)).astype(BF)


def transpose2(w):
    hi, lo = split2(w)
    unit = eye(w.shape[1])
    return dot_nt(unit, hi).astype(BF), dot_nt(unit, lo).astype(BF)


def rows3(x):
    hi, mid, lo = split3(x)
    return jnp.concatenate([hi, mid, lo, jnp.zeros_like(hi)], 0).astype(BF)


def fold3(y):
    return y[0:8] + (y[8:16] + y[16:24])


def fold2(y):
    n = y.shape[0] // 2
    return y[:n] + y[n:]


def tile_lanes(x, count):
    return jnp.concatenate([x] * count, 1)


def lanes_at(x, index):
    return jnp.take_along_axis(x, index, axis=1, mode="promise_in_bounds")


def twice(x):
    return jnp.concatenate([x, x], 0)


def kernel(
    live_any, pos_any, kind_any, neigh_any, count_any, send_any, embed_any, site_any, win_any,
    wmid_any, wout_any, contract_any, mix_any, skip_any, rone_any, rhid_any, rout_any,
    out_ref,
    live_ref, pos_ref, kind_ref, neigh_ref, count_ref, send_ref, embed_ref, site_ref, win_ref,
    wmid_ref, wout_ref, contract_ref, mix_ref, skip_ref, rone_ref, rhid_ref, rout_ref,
    s_ref, st_ref, oh_ref, oht_ref,
    snd1, rcv1, snd2, rcv2, snd3, rcv3, snd4, rcv4, ar1s, ar1r, ar2s, ar2r,
    rad_ref, radp_ref, feat_ref, hb_ref, a_ref, sel_ref, da_ref, gn_ref, d1_ref, d2_ref, hid_ref,
    bas_ref, basp_ref, wic_ref, wmc_ref, woc_ref, mixc_ref, mixt_ref, mixed_ref, dh_ref, q_ref,
    in_sem, ss1, rs1, ss2, rs2, ss3, rs3, ss4, rs4, sa1, ra1, sa2, ra2,
):
    arrays = [
        (pos_any, pos_ref), (kind_any, kind_ref), (send_any, send_ref), (neigh_any, neigh_ref),
        (count_any, count_ref), (live_any, live_ref), (embed_any, embed_ref), (site_any, site_ref),
        (win_any, win_ref), (wmid_any, wmid_ref), (wout_any, wout_ref), (contract_any, contract_ref),
        (mix_any, mix_ref), (skip_any, skip_ref), (rone_any, rone_ref), (rhid_any, rhid_ref),
        (rout_any, rout_ref),
    ]
    loads = [pltpu.make_async_copy(src, dst, in_sem.at[i]) for i, (src, dst) in enumerate(arrays)]
    for load in loads[:3]:
        load.start()

    p = lax.axis_index("gx")
    q = lax.axis_index("gy")
    n_gx = NX * NYH * NCORE
    n_gy = NZ * NYL

    def near(ox, oy):
        return (lax.rem(p + (ox + n_gx), n_gx), lax.rem(q + (oy + n_gy), n_gy))

    core = lax.rem(p, NCORE)
    y_hi = lax.rem(lax.div(p, NCORE), NYH)
    x = lax.div(p, NCORE * NYH)
    y_lo = lax.rem(q, NYL)
    z = lax.div(q, NYL)
    y = y_hi * NYL + y_lo

    def peer_a(i):
        yy = lax.rem(y + i // NCORE, NYH * NYL)
        cc = lax.rem(core + i % NCORE, NCORE)
        return ((x * NYH + lax.div(yy, NYL)) * NCORE + cc, z * NYL + lax.rem(yy, NYL))

    def peer_b(i):
        xx, zz = lax.rem(x + i // NZ, NX), lax.rem(z + i % NZ, NZ)
        return ((xx * NYH + y_hi) * NCORE + core, zz * NYL + y_lo)

    ahead = [near(ox, oy) for ox, oy in DIRS]
    barrier = pltpu.get_barrier_semaphore()

    def greet(who):
        pl.semaphore_signal(barrier, inc=1, device_id=who, device_id_type=pl.DeviceIdType.MESH)

    for who in ahead:
        greet(who)
    for load in loads[3:]:
        load.start()
    def ring(i, n):
        return min(i, n - i)

    far_a = lambda i: (-ring(i // NCORE, NYH * NYL), i)
    far_b = lambda i: (-ring(i // NZ, NX) - ring(i % NZ, NZ), i)
    peers_a = [peer_a(i) for i in sorted(range(1, NYH * NYL * NCORE), key=far_a)]
    peers_b = [peer_b(i) for i in sorted(range(1, NX * NZ), key=far_b)]
    for who in peers_a + peers_b:
        greet(who)

    def remote(src, dst, ssem, rsem, who):
        return pltpu.make_async_remote_copy(
            src_ref=src, dst_ref=dst, send_sem=ssem, recv_sem=rsem, device_id=who,
            device_id_type=pl.DeviceIdType.MESH,
        )

    half = iota((8, 128), 1) < 64
    sign = 2 * core - 1

    def arrive(source, target, ssem, rsem, first_slot):
        for i in range(4):
            o = first_slot + i
            remote(source.at[o], target.at[o], ssem.at[o], rsem.at[o], ahead[0]).wait_recv()

    def exchange(source, target, ssem, rsem, toward):
        outer = (1 - core) * 5 if toward < 0 else core * 5
        inner = core * 5 if toward < 0 else (1 - core) * 5
        order = [(outer + oy + 1, sign, toward * oy) for oy in (-1, 1, 0)]
        order += [(3, 0, -toward), (4, 0, toward)]
        order += [(inner + oy + 1, -sign, toward * oy) for oy in (-1, 1, 0)]
        return [
            remote(source(o), target.at[o], ssem.at[o], rsem.at[o], near(ox, oy)) for o, ox, oy in order
        ]

    for load in loads[:3]:
        load.wait()
    for b in range(4):
        row = send_ref[0:1, b * 128 : (b + 1) * 128]
        s_ref[:, b * 128 : (b + 1) * 128] = (iota((A, 128), 0) == row).astype(F32).astype(BF)
    kind = kind_ref[0:1, :]
    own8 = jnp.concatenate([pos_ref[...], kind.astype(F32), jnp.zeros((4, A), F32)], 0)
    own32 = rows3(own8)
    packet = fold3(dot(own32, s_ref[...]))
    for b in range(4):
        snd1[b] = packet[:, b * 128 : (b + 1) * 128]

    pl.semaphore_wait(barrier, len(ahead) + len(peers_a) + len(peers_b))
    copies1 = exchange(lambda o: snd1.at[lax.div(o, 2)], rcv1, ss1, rs1, -1)
    for copy in copies1:
        copy.start()

    for load in loads[3:]:
        load.wait()
    for k in range(K):
        row = neigh_ref[k : k + 1, :]
        oh_ref[:, k * A : (k + 1) * A] = (iota((A + G, A), 0) == row).astype(F32).astype(BF)
    unit = eye(128)
    for k in range(K):
        for b in range(5):
            block = oh_ref[b * 128 : (b + 1) * 128, k * A : (k + 1) * A]
            oht_ref[k * A : (k + 1) * A, b * 128 : (b + 1) * 128] = dot_tn(block, unit).astype(BF)
    for b in range(4):
        st_ref[b * 128 : (b + 1) * 128, :] = dot_tn(s_ref[:, b * 128 : (b + 1) * 128], unit).astype(BF)

    kinds4 = iota((16, A), 0)
    onehot16 = ((lax.rem(kinds4, 4) == kind) & (kinds4 < 12)).astype(F32).astype(BF)
    for l in range(2):
        in_h = win_ref[l].astype(BF).astype(F32)
        in_rows = jnp.concatenate([in_h, in_h, win_ref[l] - in_h, jnp.zeros_like(in_h)], 0)
        wic_ref[l] = dot_tn(in_rows.astype(BF), eye(32)).astype(BF)
        wmc_ref[l] = spread3(wmid_ref[l])
        oh_t, ol_t = split2(wout_ref[l])
        woc_ref[l] = dot_tn(jnp.concatenate([oh_t, oh_t, ol_t], 0), eye(3 * H)).astype(BF)
        parts = []
        for path in range(6):
            hi, mid, lo = split3(contract_ref[l, path])
            parts.append(jnp.concatenate([hi, mid, lo, jnp.zeros_like(hi)], 0).astype(BF))
        sel_ref[l] = dot_tn(jnp.concatenate(parts, 1), onehot16)
    mixh, mixl = split2(mix_ref[0])
    mixc_ref[...] = jnp.concatenate([mixh, mixh, mixl], 1)
    mth, mtl = transpose2(mix_ref[0])
    mixt_ref[...] = jnp.concatenate([mth, mth, mtl], 1)
    eh, em, el = split3(embed_ref[...])
    embed_rows = jnp.concatenate([eh, em, el, jnp.zeros_like(eh)], 0).astype(BF)
    embed16 = dot_tn(embed_rows, eye(16)).astype(BF)
    start_own = dot(embed16, onehot16)
    skip_start = dot3(skip_ref[0], start_own)
    read_mix = dot3(rhid_ref[...], mix_ref[1])
    read_skip = dot3(rhid_ref[...], skip_ref[1])
    rm_h, rm_l = split2(read_mix)
    rmc = jnp.concatenate([rm_h, rm_h, rm_l], 1)
    rmt = dot_tn(jnp.concatenate([rm_h, rm_h, rm_l], 0), eye(48)).astype(BF)
    rout = jnp.sum(jnp.where(iota((16, 16), 0) == iota((16, 16), 1), rout_ref[...], 0.0), axis=1, keepdims=True)
    live_row = (iota((1, A), 1) < live_ref[0]).astype(F32)
    site_row = jnp.zeros((1, A), F32)
    for s in range(4):
        site_row = jnp.where(kind == s, site_ref[0:1, s : s + 1], site_row)

    for copy in copies1:
        copy.wait()
    blocks = []
    rows8 = iota((8, 128), 0)
    for b in range(4):
        (ax, ay), (bx, by) = DIRS[2 * b], DIRS[2 * b + 1]
        shift_x = jnp.where(half, float(ax), float(bx))
        shift_y = jnp.where(half, float(ay), float(by))
        shift = jnp.where(rows8 == 0, shift_x, jnp.where(rows8 == 1, shift_y, 0.0))
        blocks.append(jnp.where(half, rcv1[2 * b], rcv1[2 * b + 1]) + shift)
    gathered = []
    for k in range(K):
        index = jnp.broadcast_to(neigh_ref[k : k + 1, :], (8, 128))
        place_in, lane = lax.shift_right_logical(index, 7), lax.bitwise_and(index, 127)
        picked = lanes_at(own8, lane)
        for b in range(4):
            picked = jnp.where(place_in == b + 1, lanes_at(blocks[b], lane), picked)
        gathered.append(picked)
    gathered = jnp.concatenate(gathered, 1)
    own_base = jnp.where(rows8 < 3, own8, 0.0)
    edge = gathered - tile_lanes(own_base, K)
    ex, ey, ez = edge[0:1], edge[1:2], edge[2:3]
    spec_row = edge[3:4]
    scaled = (ex * ex + ey * ey + ez * ez) * 0.25
    valid = jnp.concatenate([(k < count_ref[0:1, :]).astype(F32) for k in range(K)], 1)
    cut = jnp.exp(-scaled) * valid * 0.125
    offset = (scaled - iota((8, E), 0).astype(F32) * SPACING) / SPACING
    basis = jnp.exp(-0.5 * (offset * offset))
    slope = basis * (offset * (-1.0 / SPACING))
    bh = basis.astype(BF).astype(F32)
    bas_ref[...] = jnp.concatenate([bh, basis - bh, bh, jnp.zeros_like(bh)], 0).astype(BF)
    bh = slope.astype(BF).astype(F32)
    basp_ref[...] = jnp.concatenate([bh, slope - bh, bh, jnp.zeros_like(bh)], 0).astype(BF)

    def radial(l):
        pre = dot(wic_ref[l], bas_ref[...])
        sig = jax.nn.sigmoid(pre)
        act = pre * sig
        d1_ref[l] = sig + act * (1.0 - sig)
        pre = dot(wmc_ref[l], stack3(act))
        sig = jax.nn.sigmoid(pre)
        act = pre * sig
        d2_ref[l] = sig + act * (1.0 - sig)
        hid_ref[l] = act
        rad_ref[l] = dot(woc_ref[l], stack3(act * cut))

    def radial_slopes(l):
        act = dot(wic_ref[l], basp_ref[...]) * d1_ref[l]
        act = dot(wmc_ref[l], stack3(act)) * d2_ref[l]
        radp_ref[l] = dot(woc_ref[l], stack3((act - hid_ref[l]) * cut))

    radial(0)
    kinds_e = iota((16, E), 0)
    onehot_e = ((lax.rem(kinds_e, 4).astype(F32) == spec_row) & (kinds_e < 12)).astype(F32).astype(BF)
    feat_ref[0] = dot(embed16, onehot_e)
    harmonics = [
        ex, ey, ez, ex * ey, ey * ez, ex * ez, 0.5 * (ex * ex - ey * ey),
        (2.0 * ez * ez - ex * ex - ey * ey) / 6.0,
    ]
    for m in range(8):
        hb_ref[m * 8 : (m + 1) * 8, :] = jnp.broadcast_to(harmonics[m], (8, E))

    def harm(m, at):
        return twice(hb_ref[m * 8 : (m + 1) * 8, at])

    def moments(l):
        def body(block, carry):
            c0 = pl.multiple_of(block * 16, 16)
            total = None
            for k in range(K):
                at = slice(k * A, (k + 1) * A)
                h = feat_ref[l, pl.ds(c0, 16), at]
                w0 = rad_ref[l, pl.ds(c0, 16), at] * h
                w1 = rad_ref[l, pl.ds(C + c0, 16), at] * h
                w2 = rad_ref[l, pl.ds(2 * C + c0, 16), at] * h
                terms = [w0]
                terms += [w1 * harm(m, at) for m in range(3)]
                terms += [w2 * harm(m, at) for m in range(3, 8)]
                total = terms if total is None else [t + u for t, u in zip(total, terms)]
            for m in range(9):
                a_ref[l, pl.ds(m * C + c0, 16), :] = total[m]
            a0, x1, y1, z1, xy, yz, xz, u, w = total
            q1 = x1 * x1 + y1 * y1 + z1 * z1
            q2 = xy * xy + yz * yz + xz * xz + u * u + w * w
            triple = (u - w) * (x1 * x1) - (u + w) * (y1 * y1) + 2.0 * w * (z1 * z1)
            triple = triple + 2.0 * (xy * (x1 * y1) + yz * (y1 * z1) + xz * (x1 * z1))
            s = [sel_ref[l, pl.ds(path * C + c0, 16), :] for path in range(6)]
            mixed = s[0] * a0 + s[1] * (a0 * a0) + s[2] * q1 + s[3] * q2 + s[4] * (a0 * q1) + s[5] * triple
            hi, lo = split2(mixed)
            mixed_ref[pl.ds(c0, 16), :] = hi
            mixed_ref[pl.ds(C + c0, 16), :] = lo
            mixed_ref[pl.ds(2 * C + c0, 16), :] = hi
            return carry

        lax.fori_loop(0, C // 16, body, 0)

    def moment_grads(l, block, dm):
        c0 = pl.multiple_of(block * 16, 16)
        a0, x1, y1, z1, xy, yz, xz, u, w = [a_ref[l, pl.ds(m * C + c0, 16), :] for m in range(9)]
        g = [dm * sel_ref[l, pl.ds(path * C + c0, 16), :] for path in range(6)]
        q1 = x1 * x1 + y1 * y1 + z1 * z1
        g5 = 2.0 * g[5]
        dq = 2.0 * (g[2] + a0 * g[4])
        g3 = 2.0 * g[3]
        return [
            g[0] + 2.0 * (a0 * g[1]) + q1 * g[4],
            x1 * dq + g5 * ((u - w) * x1 + xy * y1 + xz * z1),
            y1 * dq + g5 * (xy * x1 - (u + w) * y1 + yz * z1),
            z1 * dq + g5 * (xz * x1 + yz * y1 + 2.0 * (w * z1)),
            xy * g3 + g5 * (x1 * y1),
            yz * g3 + g5 * (y1 * z1),
            xz * g3 + g5 * (x1 * z1),
            u * g3 + g[5] * (x1 * x1 - y1 * y1),
            w * g3 + g[5] * (2.0 * (z1 * z1) - x1 * x1 - y1 * y1),
        ]

    def weight_grads(d, at):
        w1 = d[1] * harm(0, at) + d[2] * harm(1, at) + d[3] * harm(2, at)
        w2 = d[4] * harm(3, at) + d[5] * harm(4, at) + d[6] * harm(5, at)
        return d[0], w1, w2 + (d[7] * harm(6, at) + d[8] * harm(7, at))

    def radial_grads(l):
        def body(k, carry):
            at = pl.ds(pl.multiple_of(k * A, A), A)
            hs = [harm(m, at) for m in range(8)]
            acc = [jnp.zeros((16, A), F32)] * 9
            for block in range(C // 16):
                c0 = block * 16
                d = [da_ref[m * C + c0 : m * C + c0 + 16, :] for m in range(9)]
                h = feat_ref[l, c0 : c0 + 16, at]
                w1 = rad_ref[l, C + c0 : C + c0 + 16, at] * h
                w2 = rad_ref[l, 2 * C + c0 : 2 * C + c0 + 16, at] * h
                e1 = d[1] * hs[0] + d[2] * hs[1] + d[3] * hs[2]
                e2 = d[4] * hs[3] + d[5] * hs[4] + d[6] * hs[5] + (d[7] * hs[6] + d[8] * hs[7])
                ds = d[0] * radp_ref[l, c0 : c0 + 16, at] + e1 * radp_ref[l, C + c0 : C + c0 + 16, at]
                ds = ds + e2 * radp_ref[l, 2 * C + c0 : 2 * C + c0 + 16, at]
                acc = [acc[m] + (w1 if m < 3 else w2) * d[m + 1] for m in range(8)] + [acc[8] + ds * h]
            for m in range(9):
                dh_ref[m : m + 1, at] = jnp.sum(acc[m], axis=0, keepdims=True)
            return carry

        lax.fori_loop(0, K, body, 0)
        g0, g1, g2, g3, g4, g5, g6, g7, ds = [dh_ref[m : m + 1, :] for m in range(9)]
        ds = ds * 0.5
        third = g7 * (1.0 / 3.0)
        gx = g0 + ey * g3 + ez * g5 + ex * (g6 - third + ds)
        gy = g1 + ex * g3 + ez * g4 + ey * (ds - g6 - third)
        gz = g2 + ey * g4 + ex * g5 + ez * (2.0 * third + ds)
        return jnp.concatenate([gx, gy, gz, jnp.zeros((5, E), F32)], 0)

    moments(0)
    first = dot(mixc_ref[...], mixed_ref[...]) + skip_start

    first_h, first_l = split2(first)
    first2 = jnp.concatenate([first_h, first_l], 0)
    lane64 = iota((64, 128), 1) < 64

    def pack(value, buf):
        for b in range(4):
            top = value[0:64, b * 128 : (b + 1) * 128]
            low = value[64:128, b * 128 : (b + 1) * 128]
            buf[2 * b] = jnp.where(lane64, top, pltpu.roll(low, 64, 1))
            buf[2 * b + 1] = jnp.where(lane64, pltpu.roll(top, 64, 1), low)

    def unpack(buf, b):
        one, two = buf[2 * b], buf[2 * b + 1]
        top = jnp.where(lane64, one, pltpu.roll(two, 64, 1))
        low = jnp.where(lane64, pltpu.roll(one, 64, 1), two)
        return jnp.concatenate([top, low], 0)

    def unpack_two(buf, slot):
        return jnp.concatenate([unpack(buf, slot), unpack(buf, slot + 1)], 1)

    pack(fold2(dot(first2, s_ref[...])), snd2)
    copies2 = exchange(lambda o: snd2.at[o], rcv2, ss2, rs2, -1)
    for copy in copies2:
        copy.start()

    radial(1)
    radial_slopes(0)

    def strain_body(block, carry):
        c0 = pl.multiple_of(block * 16, 16)
        j0, jx, jy, jz, jxy, jyz, jxz, ju, jw = moment_grads(0, block, 1.0)
        third = jw * (1.0 / 3.0)
        mxx, myy, mzz = ju - third, -ju - third, 2.0 * third
        total = None
        for k in range(K):
            at = slice(k * A, (k + 1) * A)
            vx, vy, vz = harm(0, at), harm(1, at), harm(2, at)
            h = feat_ref[0, pl.ds(c0, 16), at]
            e1 = jx * vx + jy * vy + jz * vz
            tx = mxx * vx + jxy * vy + jxz * vz
            ty = jxy * vx + myy * vy + jyz * vz
            tz = jxz * vx + jyz * vy + mzz * vz
            e2 = 0.5 * (tx * vx + ty * vy + tz * vz)
            u = j0 * radp_ref[0, pl.ds(c0, 16), at] + e1 * radp_ref[0, pl.ds(C + c0, 16), at]
            u = (u + e2 * radp_ref[0, pl.ds(2 * C + c0, 16), at]) * (0.5 * h)
            r1 = rad_ref[0, pl.ds(C + c0, 16), at] * h
            r2 = rad_ref[0, pl.ds(2 * C + c0, 16), at] * h
            gx = vx * u + r1 * jx + r2 * tx
            gy = vy * u + r1 * jy + r2 * ty
            gz = vz * u + r1 * jz + r2 * tz
            terms = [v * g for v in (vx, vy, vz) for g in (gx, gy, gz)]
            total = terms if total is None else [t + n for t, n in zip(total, terms)]
        for n in range(9):
            q_ref[pl.ds(n * C + c0, 16), :] = total[n]
        return carry

    lax.fori_loop(0, C // 16, strain_body, 0)
    radial_slopes(1)
    feat_ref[1] = fold2(dot(first2, oh_ref[0:A, :]))
    read_base = dot3(read_skip, first)
    energy_row = live_row * (dot3(rone_ref[...], first) + site_row)

    for group in range(2):
        pair = (1 - core) * 2 if group == 0 else core * 2
        arrive(snd2, rcv2, ss2, rs2, 2 * pair)
        gh, gl = split2(unpack_two(rcv2, pair))
        rows = pl.ds(pl.multiple_of(A + pair * 128, 128), 256)
        feat_ref[1] += fold2(dot(jnp.concatenate([gh, gl], 0), oh_ref[rows, :]))

    moments(1)
    pre = dot(rmc, mixed_ref[...]) + read_base
    sig = jax.nn.sigmoid(pre)
    act = pre * sig
    energy_row = energy_row + live_row * jnp.sum(rout * act, axis=0, keepdims=True)
    dpre = rout * live_row * (sig + act * (1.0 - sig))
    dps = stack3(dpre)
    da_ref[9 * C :, :] = dot(rmt, dps)

    def neigh_body(block, carry):
        c0 = pl.multiple_of(block * 16, 16)
        d = moment_grads(1, block, da_ref[pl.ds(9 * C + c0, 16), :])
        for m in range(9):
            da_ref[pl.ds(m * C + c0, 16), :] = d[m]
        for k in range(K):
            at = slice(k * A, (k + 1) * A)
            w0, w1, w2 = weight_grads(d, at)
            g = w0 * rad_ref[1, pl.ds(c0, 16), at]
            g = g + w1 * rad_ref[1, pl.ds(C + c0, 16), at]
            g = g + w2 * rad_ref[1, pl.ds(2 * C + c0, 16), at]
            hi, lo = split2(g)
            gn_ref[pl.ds(c0, 16), at] = hi
            gn_ref[pl.ds(C + c0, 16), at] = lo
        return carry

    lax.fori_loop(0, C // 16, neigh_body, 0)
    pack(fold2(dot(gn_ref[...], oht_ref[:, A:])), snd3)
    copies3 = exchange(lambda o: snd3.at[o], rcv3, ss3, rs3, 1)
    for copy in copies3:
        copy.start()

    own_grad = fold2(dot(gn_ref[...], oht_ref[:, 0:A]))
    rs_h, rs_l = split2(read_skip)
    own_grad = own_grad + dot_tn(jnp.concatenate([rs_h, rs_h, rs_l], 0), dps)
    o_h, o_m, o_l = split3(jnp.concatenate([rone_ref[...], jnp.zeros((7, C), F32)], 0))
    live8 = jnp.where(rows8 == 0, live_row, 0.0).astype(BF)
    own_grad = own_grad + dot_tn(o_h.astype(BF), live8)
    own_grad = own_grad + (dot_tn(o_m.astype(BF), live8) + dot_tn(o_l.astype(BF), live8))
    grad_two = radial_grads(1)
    for n in range(3):
        at = [q_ref[(3 * n + m) * C : (3 * n + m + 1) * C, :] for m in range(3)]
        moved = dot(mixc_ref[...], stack3(jnp.concatenate(at, 1)))
        for m in range(3):
            q_ref[(3 * n + m) * C : (3 * n + m + 1) * C, :] = moved[:, m * 128 : (m + 1) * 128]
    rows16, lanes16 = iota((16, 128), 0), iota((16, 128), 1)
    partial = []
    for a in range(3):
        for b in range(3):
            prod = edge[a : a + 1] * grad_two[b : b + 1]
            part = prod[:, 0:A]
            for k in range(1, K):
                part = part + prod[:, k * A : (k + 1) * A]
            partial.append(part)
    partial = jnp.concatenate(partial + [energy_row, live_row, jnp.zeros((5, A), F32)], 0)

    returned = own_grad
    for group in range(2):
        pair = core * 2 if group == 0 else (1 - core) * 2
        arrive(snd3, rcv3, ss3, rs3, 2 * pair)
        rh, rl = split2(unpack_two(rcv3, pair))
        rows = pl.ds(pl.multiple_of(pair * 128, 128), 256)
        returned = returned + fold2(dot(jnp.concatenate([rh, rl], 0), st_ref[rows, :]))
    for n in range(9):
        part = jnp.sum(returned * q_ref[n * C : (n + 1) * C, :], axis=0, keepdims=True)
        partial = partial + jnp.where(rows16 == n, part, 0.0)
    sums = jnp.sum(partial, axis=1, keepdims=True)
    total = jnp.sum(jnp.where(lanes16 == rows16, sums, 0.0), axis=0, keepdims=True)
    ar1s[...] = total

    def spread(src, dst, ssem, rsem, peers):
        copies = [remote(src, dst.at[pl.ds(i, 1)], ssem.at[i], rsem.at[i], who) for i, who in enumerate(peers)]
        for copy in copies:
            copy.start()
        return copies

    def gather_sum(base, buf, copies):
        for copy in copies:
            copy.wait_send()
        for copy in reversed(copies):
            copy.wait_recv()
        count = len(copies)
        rows = buf[...]
        rows = jnp.where(iota(rows.shape, 0) < count, rows, 0.0)
        return base + jnp.sum(rows, axis=0, keepdims=True)

    reduce1 = spread(ar1s, ar1r, sa1, ra1, peers_a)
    da_ref[9 * C :, :] = dot(mixt_ref[...], stack3(returned))

    def first_body(block, carry):
        c0 = pl.multiple_of(block * 16, 16)
        d = moment_grads(0, block, da_ref[pl.ds(9 * C + c0, 16), :])
        for m in range(9):
            da_ref[pl.ds(m * C + c0, 16), :] = d[m]
        return carry

    lax.fori_loop(0, C // 16, first_body, 0)
    grad = radial_grads(0) + grad_two

    g32 = rows3(grad)
    ghost_pos = fold3(dot(g32, oht_ref[:, A:]))
    for b in range(4):
        snd4[b] = ghost_pos[:, b * 128 : (b + 1) * 128]
    copies4 = exchange(lambda o: snd4.at[lax.div(o, 2)], rcv4, ss4, rs4, 1)
    for copy in copies4:
        copy.start()
    own_pos = fold3(dot(g32, oht_ref[:, 0:A]))
    for k in range(K):
        own_pos = own_pos - grad[:, k * A : (k + 1) * A]

    for copy in copies2 + copies3:
        copy.wait_send()
    total = gather_sum(total, ar1r, reduce1)
    ar2s[...] = total
    reduce2 = spread(ar2s, ar2r, sa2, ra2, peers_b)

    for copy in copies4:
        copy.wait()
    home = jnp.concatenate([jnp.where(half, rcv4[2 * b], rcv4[2 * b + 1]) for b in range(4)], 1)
    own_pos = own_pos + fold3(dot(rows3(home), st_ref[...]))
    out_ref[0:3, :] = -own_pos[0:3]

    total = gather_sum(total, ar2r, reduce2)
    total = total / total[:, 10:11]
    out_ref[3:4, :] = total


def finish(out_ref, energy_ref, forces_ref, stress_ref):
    forces_ref[...] = out_ref[0:3, :]
    total = out_ref[3:4, :]
    energy_ref[...] = total[:, 9:10]
    stress_ref[...] = jnp.concatenate([total[:, 0:3], total[:, 3:6], total[:, 6:9]], 0)


def per_device(
    positions, species, neighbours, counts, live_atoms, ghost_send, embed, site_energy, radial_in,
    radial_mid, radial_out, contract, mix, skip, read_one, read_hidden, read_out,
):
    vmem = pl.BlockSpec(memory_space=pltpu.VMEM)
    dma = pltpu.SemaphoreType.DMA
    operands = (
        live_atoms, positions, species.reshape(1, A), neighbours, counts.reshape(1, A),
        ghost_send.reshape(1, G), embed.T, site_energy.reshape(1, 4), radial_in.transpose(0, 2, 1),
        radial_mid, radial_out.transpose(0, 2, 1), contract.transpose(0, 2, 1, 3), mix, skip,
        read_one.reshape(1, C), read_hidden, read_out.reshape(1, 16),
    )
    result = pl.pallas_call(
        kernel,
        out_shape=pltpu.VMEM((8, A), F32),
        in_specs=[pl.BlockSpec(memory_space=pl.ANY)] * 17,
        out_specs=vmem,
        scratch_shapes=[pltpu.SMEM((1,), jnp.int32)]
        + [pltpu.VMEM(value.shape, value.dtype) for value in operands[1:]]
        + [
            pltpu.VMEM((A, G), BF),
            pltpu.VMEM((G, A), BF),
            pltpu.VMEM((A + G, E), BF),
            pltpu.VMEM((E, A + G), BF),
            pltpu.VMEM((4, 8, 128), F32),
            pltpu.VMEM((8, 8, 128), F32),
            pltpu.VMEM((8, 64, 128), F32),
            pltpu.VMEM((8, 64, 128), F32),
            pltpu.VMEM((8, 64, 128), F32),
            pltpu.VMEM((8, 64, 128), F32),
            pltpu.VMEM((4, 8, 128), F32),
            pltpu.VMEM((8, 8, 128), F32),
            pltpu.VMEM((1, 128), F32),
            pltpu.VMEM((16, 128), F32),
            pltpu.VMEM((1, 128), F32),
            pltpu.VMEM((32, 128), F32),
            pltpu.VMEM((2, 3 * C, E), F32),
            pltpu.VMEM((2, 3 * C, E), F32),
            pltpu.VMEM((2, C, E), F32),
            pltpu.VMEM((64, E), F32),
            pltpu.VMEM((2, 9 * C, A), F32),
            pltpu.VMEM((2, 6 * C, A), F32),
            pltpu.VMEM((10 * C, A), F32),
            pltpu.VMEM((2 * C, E), BF),
            pltpu.VMEM((2, H, E), F32),
            pltpu.VMEM((2, H, E), F32),
            pltpu.VMEM((2, H, E), F32),
            pltpu.VMEM((32, E), BF),
            pltpu.VMEM((32, E), BF),
            pltpu.VMEM((2, H, 32), BF),
            pltpu.VMEM((2, H, 3 * H), BF),
            pltpu.VMEM((2, 3 * C, 3 * H), BF),
            pltpu.VMEM((C, 3 * C), BF),
            pltpu.VMEM((C, 3 * C), BF),
            pltpu.VMEM((3 * C, A), BF),
            pltpu.VMEM((16, E), F32),
            pltpu.VMEM((9 * C, A), F32),
            dma((17,)),
            dma((8,)), dma((8,)), dma((8,)), dma((8,)), dma((8,)), dma((8,)), dma((8,)), dma((8,)),
            dma((15,)), dma((15,)), dma((31,)), dma((31,)),
        ],
        compiler_params=pltpu.CompilerParams(
            collective_id=0, has_side_effects=True, vmem_limit_bytes=56 * 1024 * 1024
        ),
    )(*operands)
    energy, forces, stress = pl.pallas_call(
        finish,
        out_shape=(
            jax.ShapeDtypeStruct((1, 1), F32),
            jax.ShapeDtypeStruct((3, A), F32),
            jax.ShapeDtypeStruct((3, 3), F32),
        ),
        in_specs=[vmem],
        out_specs=(vmem, vmem, vmem),
    )(pltpu.with_memory_space_constraint(result, pltpu.VMEM))
    return energy.reshape(()), forces, stress


def solution(mesh):
    both = ("gx", "gy")
    placed = (P(None, both), P(both), P(None, both), P(both), P(both), P(both)) + (P(),) * 11
    return jax.shard_map(
        per_device, mesh=mesh, in_specs=placed, out_specs=(P(), P(None, both), P()), check_vma=False
    )
```
